32 devices in a mesh: dp: 4 (over z), row: 2 (over x), col: 4 (over y, core).
Axes of the slice: x: 2, y: 2, z: 4, core: 2. Of those that a mesh axis runs over, the one named last changes fastest.
Arguments:
- images: bfloat16 [32, 729, 1152], P(('dp', 'row', 'col')), may hold values from -6 to 6
- cotangent: bfloat16 [32, 729, 1152], P(('dp', 'row', 'col')), may hold values from -6 to 6
- first_gain: float32 [1152], replicated, may hold values from 0.25 to 1.75
- first_shift: float32 [1152], replicated, may hold values from -3 to 3
- query_weight: bfloat16 [1152, 1152], P('row', 'col'), may hold values from -0.1875 to 0.1875
- query_bias: float32 [1152], P('col'), may hold values from -3 to 3
- key_weight: bfloat16 [1152, 1152], P('row', 'col'), may hold values from -0.1875 to 0.1875
- value_weight: bfloat16 [1152, 1152], P('row', 'col'), may hold values from -0.1875 to 0.1875
- value_bias: float32 [1152], P('col'), may hold values from -3 to 3
- output_weight: bfloat16 [1152, 1152], P('col', 'row'), may hold values from -0.75 to 0.75
- output_bias: float32 [1152], replicated, may hold values from -3 to 3
- second_gain: float32 [1152], replicated, may hold values from 0.1 to 1.9
- second_shift: float32 [1152], replicated, may hold values from -3 to 3
- expand_weight: bfloat16 [1152, 4304], P('row', 'col'), may hold values from -0.1875 to 0.1875
- expand_bias: float32 [4304], P('col'), may hold values from -3 to 3
- shrink_weight: bfloat16 [4304, 1152], P('col', 'row'), may hold values from -0.1875 to 0.1875
- shrink_bias: float32 [1152], replicated, may hold values from -3 to 3
Outputs:
- layer_out: bfloat16 [32, 729, 1152], P(('dp', 'row', 'col'))
- grad_images: bfloat16 [32, 729, 1152], P(('dp', 'row', 'col'))
- grad_first_gain: float32 [1152], replicated
- grad_first_shift: float32 [1152], replicated
- grad_query_weight: float32 [1152, 1152], P('row', 'col')
- grad_query_bias: float32 [1152], P('col')
- grad_key_weight: float32 [1152, 1152], P('row', 'col')
- grad_value_weight: float32 [1152, 1152], P('row', 'col')
- grad_value_bias: float32 [1152], P('col')
- grad_output_weight: float32 [1152, 1152], P('col', 'row')
- grad_output_bias: float32 [1152], replicated
- grad_second_gain: float32 [1152], replicated
- grad_second_shift: float32 [1152], replicated
- grad_expand_weight: float32 [1152, 4304], P('row', 'col')
- grad_expand_bias: float32 [4304], P('col')
- grad_shrink_weight: float32 [4304, 1152], P('col', 'row')
- grad_shrink_bias: float32 [1152], replicated
The draws below stay inside these ranges and needn't reach their ends.
All inputs are finite; a program needn't handle non-finite values.
Results may differ from the reference program's by a relative error of at most 0.038.
Values may be sent and summed in bfloat16 or wider, within the bound.
A program may use at most 448 MiB of HBM per device.

```python
import jax
import jax.numpy as jnp
from jax import lax

D = 1152
HEADS = 16
HEAD_DIM = 72
FF = 4304
L = 729
IMAGES = 32
N_ROW = 2
N_COL = 4


def level_of(rng, extent, pieces, low, top_value):
    level = 1.0
    for dim, shards_of in pieces:
        steps = jax.random.uniform(jax.random.fold_in(jax.random.fold_in(rng, 6), dim), (shards_of,), jnp.float32, low / len(pieces), top_value / len(pieces))
        level = level * jnp.repeat(jnp.exp(steps), extent[dim] // shards_of).reshape((-1,) + (1,) * (len(extent) - 1 - dim))
    return level


def noise(stream_key, dims, spread, limit, split=(), dtype=jnp.bfloat16):
    loudness = level_of(stream_key, dims, split, -0.22, 0.18) if split else 1.0
    values = jax.random.normal(stream_key, dims, jnp.float32) * spread * loudness
    return jnp.minimum(jnp.maximum(values, -limit), limit).astype(dtype)


def setup_inputs(seed: int = 0) -> dict:
    key_list = jax.random.split(jax.random.key(seed), 18)
    return {
        "images": noise(key_list[0], (IMAGES, L, D), 1.0, 6.0, ((0, 32),)),
        "cotangent": noise(key_list[1], (IMAGES, L, D), 1.0, 6.0, ((0, 32),)),
        "first_gain": jnp.clip(1.0 + 0.15 * jax.random.normal(key_list[2], (D,), jnp.float32), 0.25, 1.75),
        "first_shift": noise(key_list[3], (D,), 0.5, 3.0, (), jnp.float32),
        "query_weight": noise(key_list[4], (D, D), D ** -0.5, 0.1875, ((0, 2), (1, 4))),
        "query_bias": noise(key_list[5], (D,), 0.5, 3.0, ((0, 4),), jnp.float32),
        "key_weight": noise(key_list[6], (D, D), D ** -0.5, 0.1875, ((0, 2), (1, 4))),
        "value_weight": noise(key_list[7], (D, D), D ** -0.5, 0.1875, ((0, 2), (1, 4))),
        "value_bias": noise(key_list[8], (D,), 0.5, 3.0, ((0, 4),), jnp.float32),
        "output_weight": noise(key_list[9], (D, D), (D // 16) ** -0.5, 0.75, ((0, 4), (1, 2))),
        "output_bias": noise(key_list[10], (D,), 0.5, 3.0, (), jnp.float32),
        "second_gain": jnp.clip(1.0 + 0.18 * jax.random.normal(key_list[11], (D,), jnp.float32), 0.1, 1.9),
        "second_shift": noise(key_list[12], (D,), 0.5, 3.0, (), jnp.float32),
        "expand_weight": noise(key_list[13], (D, FF), D ** -0.5, 0.1875, ((0, 2), (1, 4))),
        "expand_bias": noise(key_list[14], (FF,), 0.5, 3.0, ((0, 4),), jnp.float32),
        "shrink_weight": noise(key_list[15], (FF, D), (FF // 4) ** -0.5, 0.1875, ((0, 4), (1, 2))),
        "shrink_bias": noise(key_list[16], (D,), 0.5, 3.0, (), jnp.float32),
    }


EPS = 1e-06

def rounded(value):
    return lax.optimization_barrier(value.astype(jnp.bfloat16))

def blocked(pairs, parts):
    total = None
    for left, right in pairs:
        length = left.shape[0]
        inner_size = left.shape[1] // parts
        left3 = left.astype(jnp.float32).reshape(length, parts, inner_size)
        right3 = right.astype(jnp.float32).reshape(parts, inner_size, right.shape[1])
        term = jnp.einsum('lpk,pkn->pln', left3, right3)
        total = term if total is None else total + term
    return lax.optimization_barrier(jnp.sum(rounded(total).astype(jnp.float32), axis=0))

def norm_forward(stream, gain, shift):
    average = lax.optimization_barrier(jnp.mean(stream, axis=-1, keepdims=True))
    second = lax.optimization_barrier(jnp.mean(stream * stream, axis=-1, keepdims=True))
    inverse = lax.rsqrt(second - average * average + EPS)
    normed = (stream - average) * inverse
    return (normed, inverse, rounded(normed * gain + shift))

def norm_backward(grad_out, normed, inverse, gain):
    scaled = grad_out * gain
    first = lax.optimization_barrier(jnp.mean(scaled, axis=-1, keepdims=True))
    second = lax.optimization_barrier(jnp.mean(scaled * normed, axis=-1, keepdims=True))
    return inverse * (scaled - first - normed * second)

def gelu_tanh(value):
    return jax.nn.gelu(value, approximate=True)

def split_heads(block):
    return block.astype(jnp.float32).reshape(block.shape[0], HEADS, HEAD_DIM)

def attention_scores(queries, key_rows):
    return jnp.einsum('qhd,khd->hqk', split_heads(queries), split_heads(key_rows)) * HEAD_DIM ** (-0.5)

def attention_forward(queries, key_rows, value_rows):
    scores = attention_scores(queries, key_rows)
    peak = lax.optimization_barrier(jnp.max(scores, axis=-1, keepdims=True))
    log_total = peak + jnp.log(lax.optimization_barrier(jnp.sum(jnp.exp(scores - peak), axis=-1, keepdims=True)))
    attention = rounded(jnp.exp(scores - log_total)).astype(jnp.float32)
    attended = jnp.einsum('hqk,khd->qhd', attention, split_heads(value_rows))
    return (rounded(attended.reshape(queries.shape[0], D)), log_total)

def attention_backward(queries, key_rows, value_rows, attended, log_total, grad_attended):
    scores = attention_scores(queries, key_rows)
    attention = jnp.exp(scores - log_total)
    attention_bf = rounded(attention).astype(jnp.float32)
    grad_heads = split_heads(grad_attended)
    grad_probs = jnp.einsum('qhd,khd->hqk', grad_heads, split_heads(value_rows))
    delta = jnp.einsum('qhd,qhd->hq', grad_heads, split_heads(attended))[..., None]
    grad_scores = rounded(attention * (grad_probs - delta)).astype(jnp.float32)
    scale = HEAD_DIM ** (-0.5)
    grad_queries = jnp.einsum('hqk,khd->qhd', grad_scores, split_heads(key_rows)) * scale
    grad_keys = jnp.einsum('hqk,qhd->khd', grad_scores, split_heads(queries)) * scale
    grad_values = jnp.einsum('hqk,qhd->khd', attention_bf, grad_heads)
    length = queries.shape[0]
    return (grad_queries.reshape(length, D), grad_keys.reshape(length, D), grad_values.reshape(length, D))

def outer(left, right):
    return jnp.dot(left.T, right, preferred_element_type=jnp.float32)

def layer_image(params, image, cotangent):
    first_gain, first_shift, query_weight, query_bias, key_weight, value_weight, value_bias, output_weight, output_bias, second_gain, second_shift, expand_weight, expand_bias, shrink_weight, shrink_bias = params
    stream = image.astype(jnp.float32)
    normed1, inverse1, input1 = norm_forward(stream, first_gain, first_shift)
    queries = rounded(blocked([(input1, query_weight)], N_ROW) + query_bias)
    key_rows = rounded(blocked([(input1, key_weight)], N_ROW))
    value_rows = rounded(blocked([(input1, value_weight)], N_ROW) + value_bias)
    attended, log_total = attention_forward(queries, key_rows, value_rows)
    middle = stream + blocked([(attended, output_weight)], N_COL) + output_bias
    normed2, inverse2, input2 = norm_forward(middle, second_gain, second_shift)
    before = blocked([(input2, expand_weight)], N_ROW) + expand_bias
    hidden = rounded(gelu_tanh(before))
    result = middle + blocked([(hidden, shrink_weight)], N_COL) + shrink_bias
    grad_result = cotangent.astype(jnp.float32)
    grad_hidden = blocked([(cotangent, shrink_weight.T)], N_ROW)
    gelu_back = jax.vjp(gelu_tanh, before)[1]
    grad_before = gelu_back(grad_hidden)[0]
    grad_before_bf = rounded(grad_before)
    grad_input2 = blocked([(grad_before_bf, expand_weight.T)], N_COL)
    grad_middle = grad_result + norm_backward(grad_input2, normed2, inverse2, second_gain)
    grad_middle_bf = rounded(grad_middle)
    grad_attended = rounded(blocked([(grad_middle_bf, output_weight.T)], N_ROW))
    grad_queries, grad_keys, grad_values = attention_backward(queries, key_rows, value_rows, attended, log_total, grad_attended)
    queries_bf = rounded(grad_queries)
    keys_bf = rounded(grad_keys)
    values_bf = rounded(grad_values)
    grad_input1 = blocked([(queries_bf, query_weight.T), (keys_bf, key_weight.T), (values_bf, value_weight.T)], N_COL)
    grad_stream = grad_middle + norm_backward(grad_input1, normed1, inverse1, first_gain)
    grads = (lax.optimization_barrier(jnp.sum(grad_input1 * normed1, axis=0)), lax.optimization_barrier(jnp.sum(grad_input1, axis=0)), outer(input1, queries_bf), lax.optimization_barrier(jnp.sum(grad_queries, axis=0)), outer(input1, keys_bf), outer(input1, values_bf), lax.optimization_barrier(jnp.sum(grad_values, axis=0)), outer(attended, grad_middle_bf), lax.optimization_barrier(jnp.sum(grad_middle, axis=0)), lax.optimization_barrier(jnp.sum(grad_input2 * normed2, axis=0)), lax.optimization_barrier(jnp.sum(grad_input2, axis=0)), outer(input2, grad_before_bf), lax.optimization_barrier(jnp.sum(grad_before, axis=0)), outer(hidden, cotangent), lax.optimization_barrier(jnp.sum(grad_result, axis=0)))
    return (grads, result.astype(jnp.bfloat16), grad_stream.astype(jnp.bfloat16))

def reference(images, cotangent, first_gain, first_shift, query_weight, query_bias, key_weight, value_weight, value_bias, output_weight, output_bias, second_gain, second_shift, expand_weight, expand_bias, shrink_weight, shrink_bias):
    params = (first_gain, first_shift, query_weight, query_bias, key_weight, value_weight, value_bias, output_weight, output_bias, second_gain, second_shift, expand_weight, expand_bias, shrink_weight, shrink_bias)
    initial = tuple((jnp.zeros(param.shape, jnp.float32) for param in params))

    def step(carry, pair):
        grads, result, grad_stream = layer_image(params, pair[0], pair[1])
        return (tuple((held + fresh for held, fresh in zip(carry, grads))), (result, grad_stream))
    totals, (layer_out, grad_images) = lax.scan(step, initial, (images, cotangent))
    return (layer_out, grad_images, totals[0], totals[1], totals[2], totals[3], totals[4], totals[5], totals[6], totals[7], totals[8], totals[9], totals[10], totals[11], totals[12], totals[13], totals[14])
```

```python
import functools, math
import jax
import jax.numpy as jnp
from jax import lax
from jax.experimental import pallas as pl
from jax.experimental.pallas import tpu as pltpu
from jax.sharding import PartitionSpec as P

HEAD = 72
LANE = 128
F32, BF16 = jnp.float32, jnp.bfloat16
NT = (((1,), (1,)), ((), ()))
TN = (((0,), (0,)), ((), ()))
ANY = pl.BlockSpec(memory_space=pl.ANY)
VM = pl.BlockSpec(memory_space=pltpu.VMEM)
VLIM = 60 * 1024 * 1024


def dot(a, b):
    return jnp.dot(a, b, preferred_element_type=F32)


def dot_nt(a, b):
    return lax.dot_general(a, b, NT, preferred_element_type=F32)


def dot_tn(a, b):
    return lax.dot_general(a, b, TN, preferred_element_type=F32)


def tiles(total, width, body):
    count = -(-total // width)

    def step(i, _):
        body(pl.multiple_of(jnp.minimum(i * width, total - width), LANE))
        return 0

    lax.fori_loop(0, count, step, 0)


class Copies:
    def __init__(self, sems):
        self.sems, self.n = sems, 0

    def __call__(self, src, dst):
        copy = pltpu.make_async_copy(src, dst, self.sems.at[self.n])
        self.n += 1
        copy.start()
        return copy


def load_rows(copies, blocks, dst):
    n = len(blocks)
    size = blocks[0].shape[0]
    me = lax.axis_index("row")
    out = []
    for s, block in enumerate(blocks):
        row = lax.rem(me - s + n, n)
        out.append(copies(block, dst.at[pl.ds(pl.multiple_of(row * size, 16), size), :]))
    return out


def wait(copies):
    for copy in copies:
        copy.wait()


GC = math.sqrt(2.0 / math.pi)


def ff_kernel(n, *refs):
    in2, cot, bias = refs[:3]
    eb, sb = refs[3 : 3 + n], refs[3 + n : 3 + 2 * n]
    res_in, gi_in = refs[3 + 2 * n : 5 + 2 * n]
    hid_o, gb_o, res_o, gi_o, db = refs[5 + 2 * n : 10 + 2 * n]
    in2_v, cot_v, e_v, s_v, hid_v, gb_v, res_v, gi_v, sems = refs[10 + 2 * n :]
    c = Copies(sems)
    first = [c(in2, in2_v)] + load_rows(c, eb, e_v)
    second = [c(cot, cot_v)] + load_rows(c, sb, s_v)
    third = [c(res_in, res_v), c(gi_in, gi_v)]
    wait(first)
    wait(second)
    width = e_v.shape[1]

    def hidden_tile(at):
        cols = pl.ds(at, 256)
        b = dot(in2_v[...], e_v[:, cols]) + bias[:, cols]
        sq = b * b
        t = jnp.tanh(GC * b * (1.0 + 0.044715 * sq))
        half = 0.5 * (1.0 + t)
        hid_v[:, cols] = (b * half).astype(BF16)
        slope = half + (0.5 * GC) * b * (1.0 - t * t) * (1.0 + (3 * 0.044715) * sq)
        g = dot(cot_v[...], s_v[:, cols]) * slope
        gb_v[:, cols] = g.astype(BF16)
        db[:, cols] = jnp.sum(g, axis=0, keepdims=True)

    tiles(width, 256, hidden_tile)
    out = [c(hid_v, hid_o), c(gb_v, gb_o)]
    wait(third)

    for a in range(0, width, 256):
        w = min(256, width - a)
        res_v[:, a : a + w] += dot_nt(hid_v[...], s_v[a : a + w, :])
        gi_v[:, a : a + w] += dot_nt(gb_v[...], e_v[a : a + w, :])
    out += [c(res_v, res_o), c(gi_v, gi_o)]
    wait(out)


def ff(in2, cot, bias, eb, sb, res, gi):
    n, (t, d) = len(eb), in2.shape
    w = eb[0].shape[1]
    o = jax.ShapeDtypeStruct
    return pl.pallas_call(
        functools.partial(ff_kernel, n),
        name="ff",
        in_specs=[ANY, ANY, VM] + [ANY] * (2 * n + 2),
        out_specs=[ANY] * 4 + [VM],
        out_shape=[o((t, w), BF16), o((t, w), BF16), o((t, d), F32), o((t, d), F32), o((1, w), F32)],
        scratch_shapes=[
            pltpu.VMEM((t, d), BF16), pltpu.VMEM((t, d), BF16),
            pltpu.VMEM((d, w), BF16), pltpu.VMEM((d, w), BF16),
            pltpu.VMEM((t, w), BF16), pltpu.VMEM((t, w), BF16),
            pltpu.VMEM((t, d), F32), pltpu.VMEM((t, d), F32),
            pltpu.SemaphoreType.DMA((2 * n + 8,)),
        ],
        input_output_aliases={3 + 2 * n: 2, 4 + 2 * n: 3},
        compiler_params=pltpu.CompilerParams(vmem_limit_bytes=VLIM),
        cost_estimate=pl.CostEstimate(flops=8 * t * d * w, bytes_accessed=4 * d * w + 12 * t * d + 8 * t * d, transcendentals=t * w),
    )(in2, cot, bias, *eb, *sb, res, gi)


def lanes(shape):
    return lax.broadcasted_iota(jnp.int32, shape, 1)


def pick(ref, at):
    base = at // LANE * LANE
    window = ref[:, base : base + 2 * LANE]
    shift = at - base
    if shift:
        window = pltpu.roll(window, 2 * LANE - shift, 1)
    return window[:, :LANE]


def put(ref, at, value):
    base = min(at // LANE * LANE, ref.shape[1] - 2 * LANE)
    wide = jnp.concatenate((value, jnp.zeros_like(value)), axis=1)
    if at - base:
        wide = pltpu.roll(wide, at - base, 1)
    ref[:, base : base + 2 * LANE] += wide


def split3(value):
    hi = value.astype(BF16).astype(F32)
    rest = value - hi
    mid = rest.astype(BF16).astype(F32)
    return hi, mid, rest - mid


SCALE = HEAD ** -0.5
C2 = SCALE * math.log2(math.e)
PENALTY = -1e30


def attn_kernel(n, heads, length, chunk, *refs):
    in1, bias = refs[:2]
    ab = refs[2 : 2 + n]
    mid_in = refs[2 + n]
    q_o, k_o, v_o, att_o, mid_o = refs[3 + n : 8 + n]
    in1_v, a_v, qkv_v, q_v, k_v, v_v, o_v, att_v, mid_v, attb_v, sems = refs[8 + n :]
    t = in1_v.shape[0]
    c = Copies(sems)
    first = [c(in1, in1_v)] + load_rows(c, ab, a_v)
    third = [c(mid_in, mid_v)]
    wait(first)

    def proj(at):
        cols = pl.ds(at, 256)
        qkv_v[:, cols] = dot(in1_v[...], a_v[:, cols]) + bias[:, cols]

    tiles(7 * LANE, 256, proj)
    lane = lanes((t, LANE))
    row = lax.broadcasted_iota(jnp.int32, (t, LANE), 0)
    tail_k = jnp.where(lane < HEAD + 3, 1.0, jnp.where((lane == HEAD + 3) & (row >= length), 1.0, 0.0))
    tail_q = jnp.where(lane == HEAD + 3, PENALTY, 0.0)
    tail_v = jnp.where(lane < HEAD + 2, 1.0, 0.0)
    part = HEAD * heads
    for j in range(heads):
        q_v[j] = jnp.where(lane < HEAD, pick(qkv_v, HEAD * j), tail_q).astype(BF16)
        k_v[j] = jnp.where(lane < HEAD, pick(qkv_v, part + HEAD * j), tail_k).astype(BF16)
        v_v[j] = jnp.where(lane < HEAD, pick(qkv_v, 2 * part + HEAD * j), tail_v).astype(BF16)
    out = [c(k_v, k_o), c(v_v, v_o)]

    def head(j, _):
        def rows(i, _):
            at = pl.ds(pl.multiple_of(i * chunk, 16), chunk)
            q = q_v[j, at, :]
            s = dot_nt(q, k_v[j])
            m = jnp.max(s, axis=1, keepdims=True)
            p = jnp.exp2((s - m) * C2)
            o = dot(p.astype(BF16), v_v[j])
            ln = lanes((chunk, LANE))
            total = jnp.sum(jnp.where(ln == HEAD, o, 0.0), axis=1, keepdims=True)
            o_v[j, at, :] = jnp.where(ln < HEAD, o / total, 0.0)
            hi, mid, lo = split3(m + jnp.log2(total) * (1.0 / C2))
            aug = jnp.where(ln == HEAD, -hi, jnp.where(ln == HEAD + 1, -mid, jnp.where(ln == HEAD + 2, -lo, q.astype(F32))))
            q_v[j, at, :] = aug.astype(BF16)
            return 0

        return lax.fori_loop(0, t // chunk, rows, 0)

    lax.fori_loop(0, heads, head, 0)
    out += [c(q_v, q_o)]
    att_v[...] = jnp.zeros_like(att_v)
    for j in range(heads):
        put(att_v, 3 * LANE - part + HEAD * j, o_v[j])
    attb_v[...] = att_v[...].astype(BF16)
    out += [c(attb_v, att_o)]
    wait(third)
    d = mid_v.shape[1]
    for a in range(0, d, 256):
        w = min(256, d - a)
        mid_v[:, a : a + w] += dot_nt(attb_v[...], a_v[a : a + w, 6 * LANE : 9 * LANE])
    out += [c(mid_v, mid_o)]
    wait(out)


def attn(in1, bias, ab, mid, length, chunk=368):
    n, (t, d) = len(ab), in1.shape
    w = ab[0].shape[1]
    heads = w // 4 // HEAD
    o = jax.ShapeDtypeStruct
    hs = (heads, t, LANE)
    return pl.pallas_call(
        functools.partial(attn_kernel, n, heads, length, chunk),
        name="attn",
        in_specs=[ANY, VM] + [ANY] * (n + 1),
        out_specs=[ANY] * 5,
        out_shape=[o(hs, BF16)] * 3 + [o((t, 3 * LANE), BF16), o((t, d), F32)],
        scratch_shapes=[
            pltpu.VMEM((t, d), BF16), pltpu.VMEM((d, w), BF16), pltpu.VMEM((t, 8 * LANE), F32),
            pltpu.VMEM(hs, BF16), pltpu.VMEM(hs, BF16), pltpu.VMEM(hs, BF16), pltpu.VMEM(hs, F32),
            pltpu.VMEM((t, 3 * LANE), F32), pltpu.VMEM((t, d), F32), pltpu.VMEM((t, 3 * LANE), BF16),
            pltpu.SemaphoreType.DMA((n + 8,)),
        ],
        input_output_aliases={2 + n: 4},
        compiler_params=pltpu.CompilerParams(vmem_limit_bytes=VLIM),
        cost_estimate=pl.CostEstimate(flops=2 * t * d * w + 8 * heads * t * t * LANE, bytes_accessed=2 * d * w + 10 * t * d, transcendentals=heads * t * t),
    )(in1, bias, *ab, mid)


def back_kernel(n, heads, chunk, *refs):
    gm = refs[0]
    ab = refs[1 : 1 + n]
    q_i, k_i, v_i, att_i, gi_in = refs[1 + n : 6 + n]
    dqkv_o, gi_o, db = refs[6 + n : 9 + n]
    gm_v, a_v, ga_v, q_v, k_v, v_v, g_v, att_v, ds_v, dq_v, dk_v, dv_v, pack_v, packb_v, gi_v, sems = refs[9 + n :]
    t = gm_v.shape[0]
    c = Copies(sems)
    first = [c(gm, gm_v)] + load_rows(c, ab, a_v)
    second = [c(att_i, att_v), c(q_i, q_v), c(k_i, k_v), c(v_i, v_v)]
    third = [c(gi_in, gi_v)]
    wait(first)
    ga_v[...] = dot(gm_v[...], a_v[:, 6 * LANE : 9 * LANE])
    lane = lanes((t, LANE))
    part = HEAD * heads
    wait(second)
    att = pack_v.at[:, : 3 * LANE]
    att[...] = att_v[...].astype(F32)
    for j in range(heads):
        at = 3 * LANE - part + HEAD * j
        base = min(at // LANE * LANE, LANE)
        def grab(ref):
            window = ref[:, base : base + 2 * LANE]
            return pltpu.roll(window, 2 * LANE - (at - base), 1)[:, :LANE] if at > base else window[:, :LANE]
        g = jnp.where(lane < HEAD, grab(ga_v), 0.0).astype(BF16).astype(F32)
        delta = jnp.sum(g * grab(att), axis=1, keepdims=True)
        hi = delta.astype(BF16).astype(F32)
        g_v[j] = jnp.where(lane == HEAD, -hi, jnp.where(lane == HEAD + 1, hi - delta, g)).astype(BF16)

    def head(j, _):
        def rows(i, _):
            at = pl.ds(pl.multiple_of(i * chunk, 16), chunk)
            p = jnp.exp2(dot_nt(k_v[j, at, :], q_v[j]) * C2)
            pb = p.astype(BF16)
            ds = (p * dot_nt(v_v[j, at, :], g_v[j])).astype(BF16)
            dv_v[j, at, :] = dot(pb, g_v[j])
            dk_v[j, at, :] = dot(ds, q_v[j]) * SCALE
            ds_v[at, :] = ds
            return 0

        lax.fori_loop(0, t // chunk, rows, 0)
        dq_v[j] = dot_tn(ds_v[...], k_v[j]) * SCALE
        return 0

    lax.fori_loop(0, heads, head, 0)
    pack_v[...] = jnp.zeros_like(pack_v)
    for j in range(heads):
        put(pack_v, HEAD * j, jnp.where(lane < HEAD, dq_v[j], 0.0))
        put(pack_v, part + HEAD * j, jnp.where(lane < HEAD, dk_v[j], 0.0))
        put(pack_v, 2 * part + HEAD * j, jnp.where(lane < HEAD, dv_v[j], 0.0))
    db[...] = jnp.sum(pack_v[...], axis=0, keepdims=True)
    packb_v[...] = pack_v[...].astype(BF16)
    out = [c(packb_v, dqkv_o)]
    wait(third)
    d = gi_v.shape[1]
    for a in range(0, d, 256):
        w = min(256, d - a)
        gi_v[:, a : a + w] += dot_nt(packb_v[...], a_v[a : a + w, : 7 * LANE])
    out += [c(gi_v, gi_o)]
    wait(out)


def back(gm, ab, q, k, v, att, gi, chunk=368):
    n, (t, d) = len(ab), gm.shape
    w = ab[0].shape[1]
    heads = q.shape[0]
    o = jax.ShapeDtypeStruct
    hs = (heads, t, LANE)
    return pl.pallas_call(
        functools.partial(back_kernel, n, heads, chunk),
        name="back",
        in_specs=[ANY] * (n + 6),
        out_specs=[ANY] * 2 + [VM],
        out_shape=[o((t, 7 * LANE), BF16), o((t, d), F32), o((1, 7 * LANE), F32)],
        scratch_shapes=[
            pltpu.VMEM((t, d), BF16), pltpu.VMEM((d, w), BF16), pltpu.VMEM((t, 3 * LANE), F32),
            pltpu.VMEM(hs, BF16), pltpu.VMEM(hs, BF16), pltpu.VMEM(hs, BF16), pltpu.VMEM(hs, BF16),
            pltpu.VMEM((t, 3 * LANE), BF16), pltpu.VMEM((t, t), BF16),
            pltpu.VMEM(hs, F32), pltpu.VMEM(hs, F32), pltpu.VMEM(hs, F32),
            pltpu.VMEM((t, 7 * LANE), F32), pltpu.VMEM((t, 7 * LANE), BF16), pltpu.VMEM((t, d), F32),
            pltpu.SemaphoreType.DMA((n + 8,)),
        ],
        input_output_aliases={5 + n: 1},
        compiler_params=pltpu.CompilerParams(vmem_limit_bytes=VLIM),
        cost_estimate=pl.CostEstimate(flops=2 * t * d * w + 20 * heads * t * t * LANE, bytes_accessed=2 * d * w + 16 * t * d, transcendentals=heads * t * t),
    )(gm, *ab, q, k, v, att, gi)


def grads_kernel(n, groups, *refs):
    k = len(groups)
    ins = refs[: 4 * k]
    outs = refs[4 * k : 4 * k + n]
    scratch = refs[4 * k + n :]
    lhs, rhs = scratch[: 2 * k], scratch[2 * k : 4 * k]
    acc, tile_v, sems, osem = scratch[4 * k :]
    c = Copies(sems)
    cps = []
    for i in range(k):
        cps += [c(ins[4 * i + u], (lhs if u < 2 else rhs)[2 * i + u % 2]) for u in range(4)]
    wait(cps)
    size = outs[0].shape[0]
    me = lax.axis_index("row")

    def step(s, _):
        slot = lax.rem(s, 2)
        row = pl.multiple_of(lax.rem(me + s, n) * size, 16)
        rows = pl.ds(row, size)

        @pl.when(s >= 2)
        def _():
            pltpu.make_async_copy(tile_v.at[slot], outs[0], osem.at[slot]).wait()

        if k == 1:
            def body(at):
                cols = pl.ds(at, 256)
                tile_v[slot, :, cols] = (
                    dot(lhs[0][rows, :], rhs[0][:, cols]) + dot(lhs[1][rows, :], rhs[1][:, cols])
                ).astype(BF16)

            tiles(groups[0][1], 256, body)
        else:
            for i, (start, width) in enumerate(groups):
                done = 0 if i == 0 else groups[i - 1][0] + groups[i - 1][1]
                for a in range(0, width, 256):
                    w = min(256, width - a)
                    value = dot(lhs[2 * i][rows, :], rhs[2 * i][:, a : a + w]) + dot(
                        lhs[2 * i + 1][rows, :], rhs[2 * i + 1][:, a : a + w]
                    )
                    at = start + a
                    if at < done:
                        o = done - at
                        value = jnp.concatenate((value[:, :o] + acc[:, at : at + o], value[:, o:]), axis=1) if o < w else value + acc[:, at : at + w]
                    acc[:, at : at + w] = value
            tile_v[slot] = acc[...].astype(BF16)
        for u in range(n):
            @pl.when(s == u)
            def _():
                pltpu.make_async_copy(tile_v.at[slot], outs[u], osem.at[slot]).start()
        return 0

    lax.fori_loop(0, n, step, 0)
    for u in range(max(0, n - 2), n):
        pltpu.make_async_copy(tile_v.at[u % 2], outs[u], osem.at[u % 2]).wait()


def grads(n, terms, width):
    k = len(terms)
    groups = tuple((term[0], term[3].shape[1]) for term in terms)
    flat = [array for term in terms for array in term[1:]]
    d, t = terms[0][1].shape
    size = d // n
    scratch = [pltpu.VMEM(term[1].shape, BF16) for term in terms for _ in range(2)]
    scratch += [pltpu.VMEM(term[3].shape, BF16) for term in terms for _ in range(2)]
    flops = sum(4 * d * t * w for _, w in groups)
    return pl.pallas_call(
        functools.partial(grads_kernel, n, groups),
        name="grads",
        in_specs=[ANY] * (4 * k),
        out_specs=[ANY] * n,
        out_shape=[jax.ShapeDtypeStruct((size, width), BF16)] * n,
        scratch_shapes=scratch + [
            pltpu.VMEM((size, width if k > 1 else LANE), F32), pltpu.VMEM((2, size, width), BF16),
            pltpu.SemaphoreType.DMA((4 * k,)), pltpu.SemaphoreType.DMA((2,)),
        ],
        compiler_params=pltpu.CompilerParams(vmem_limit_bytes=VLIM),
        cost_estimate=pl.CostEstimate(flops=flops, bytes_accessed=2 * d * width + 8 * t * d, transcendentals=0),
    )(*flat)


def hop_row(value, shift, size):
    return lax.ppermute(value, "row", [(i, (i + shift) % size) for i in range(size)])


def hop_col(value, flip):
    return lax.ppermute(value, "col", [(i, i ^ flip) for i in range(4)])


def hop_dp(value, flip):
    return lax.ppermute(value, "dp", [(i, i ^ flip) for i in range(4)])


CORE, SIDE = 1, 2


def gather(block, n, by_row):
    own = [block] + [hop_row(block, s, n) for s in range(1, n)]
    side = [hop_col(block, SIDE)]
    for s in range(1, n):
        side.append(hop_row(side[0], s, n) if by_row else hop_col(own[s], SIDE))
    return [own, side, [hop_col(b, CORE) for b in own], [hop_col(b, CORE) for b in side]]


def add(a, b):
    return (a.astype(F32) + b.astype(F32)).astype(BF16)


def scatter(own, side, n, row_first):
    def over_row(parts):
        total = parts[0]
        for s in range(1, n):
            total = add(total, hop_row(parts[s], s, n))
        return total

    if row_first:
        total = add(over_row(own), hop_col(over_row(side), SIDE))
    else:
        total = over_row([add(a, hop_col(b, SIDE)) for a, b in zip(own, side)])
    half = total.shape[0] // 2
    z = lax.axis_index("dp")
    low = lax.rem(z, 2)
    mine = lax.dynamic_slice_in_dim(total, low * half, half, 0)
    theirs = lax.dynamic_slice_in_dim(total, (1 - low) * half, half, 0)
    mine = add(mine, hop_dp(theirs, 1))
    mine = add(mine, hop_dp(mine, 2))
    theirs = hop_dp(mine, 1)
    return jnp.where(low == 0, jnp.concatenate((mine, theirs)), jnp.concatenate((theirs, mine)))


def norm(stream, gain, shift):
    average = jnp.mean(stream, axis=-1, keepdims=True)
    second = jnp.mean(stream * stream, axis=-1, keepdims=True)
    inverse = lax.rsqrt(second - average * average + EPS)
    return average, inverse, ((stream - average) * inverse * gain + shift).astype(BF16)


def norm_back(grad, normed, inverse, gain):
    scaled = grad * gain
    first = jnp.mean(scaled, axis=-1, keepdims=True)
    second = jnp.mean(scaled * normed, axis=-1, keepdims=True)
    return inverse * (scaled - first - normed * second)


EPS = 1e-6


def layer(n, images, cotangent, first_gain, first_shift, query_weight, query_bias, key_weight, value_weight, value_bias,
          output_weight, output_bias, second_gain, second_shift, expand_weight, expand_bias, shrink_weight, shrink_bias):
    length, d = images.shape[1:]
    t = -(-length // 16) * 16
    part, ff_part = query_weight.shape[1], expand_weight.shape[1]
    wide = 4 * part
    pad_ff = ((0, 0), (0, wide - ff_part))
    a_own = jnp.concatenate((query_weight, key_weight, value_weight, output_weight.T), axis=1)
    e_own = jnp.pad(expand_weight, pad_ff)
    s_own = jnp.pad(shrink_weight.T, pad_ff)
    zeros = jnp.zeros((part,), F32)
    bias_own = jnp.stack((jnp.concatenate((query_bias, zeros, value_bias, zeros)), jnp.pad(expand_bias, pad_ff[1:])))
    a_all = gather(a_own, n, True)
    bias_side = hop_col(bias_own, SIDE)
    biases = [bias_own, bias_side, hop_col(bias_own, CORE), hop_col(bias_side, CORE)]
    e_all = gather(e_own, n, True)
    s_all = gather(s_own, n, False)

    pad_t = ((0, t - length), (0, 0))
    stream = jnp.pad(images[0], pad_t).astype(F32)
    cot = jnp.pad(cotangent[0], pad_t)
    cot_t = cot.T
    cot_t2 = hop_col(cot_t, CORE)
    average1, inverse1, input1 = norm(stream, first_gain, first_shift)
    in1_t = input1.T
    in1_t2 = hop_col(in1_t, CORE)

    order = (0, 2, 1, 3)
    kept = {}
    middle = stream + output_bias
    for slot in order:
        *kept[slot], middle = attn(input1, biases[slot][:1], a_all[slot], middle, length)
    average2, inverse2, input2 = norm(middle, second_gain, second_shift)
    in2_t = input2.T
    in2_t2 = hop_col(in2_t, CORE)
    result = middle + shrink_bias
    grad2 = jnp.zeros((t, d), F32)
    hidden, before, expand_sums = {}, {}, {}
    for slot in order:
        hidden[slot], before[slot], result, grad2, expand_sums[slot] = ff(
            input2, cot, biases[slot][1:], e_all[slot], s_all[slot], result, grad2)
    ge, gs = [], []
    for slot in (0, 1):
        ge.append(grads(n, [(0, in2_t, in2_t2, before[slot], hop_col(before[slot + 2], CORE))], wide))
        gs.append(grads(n, [(0, cot_t, cot_t2, hidden[slot], hop_col(hidden[slot + 2], CORE))], wide))
    ge = scatter(ge[0], ge[1], n, True)
    gs = scatter(gs[0], gs[1], n, False)

    cot32 = cot.astype(F32)
    normed2 = (middle - average2) * inverse2
    grad_middle = cot32 + norm_back(grad2, normed2, inverse2, second_gain)
    gm = grad_middle.astype(BF16)
    gm_t = gm.T
    gm_t2 = hop_col(gm_t, CORE)
    grad1 = jnp.zeros((t, d), F32)
    joined, joined_sums = {}, {}
    for slot in (2, 0, 3, 1):
        q, k, v, att = kept[slot]
        joined[slot], grad1, joined_sums[slot] = back(gm, a_all[slot], q, k, v, att, grad1)
    ga = []
    for slot in (0, 1):
        ga.append(grads(n, [
            (0, in1_t, in1_t2, joined[slot], hop_col(joined[slot + 2], CORE)),
            (wide - 384, gm_t, gm_t2, kept[slot][3], hop_col(kept[slot + 2][3], CORE)),
        ], wide))
    ga = scatter(ga[0], ga[1], n, True)
    normed1 = (stream - average1) * inverse1
    grad_stream = grad_middle + norm_back(grad1, normed1, inverse1, first_gain)

    features = jnp.stack([jnp.sum(v, axis=0) for v in (
        grad1 * normed1, grad1, grad_middle, grad2 * normed2, grad2, cot32)])
    sums = {s: jnp.concatenate((jnp.pad(joined_sums[s], ((0, 0), (0, wide - joined_sums[s].shape[1]))), expand_sums[s])) for s in range(4)}
    pair = jnp.concatenate((features, sums[0], sums[1])) + hop_col(jnp.concatenate((features, sums[2], sums[3])), CORE)
    one = pair[:8] + hop_col(jnp.concatenate((pair[:6], pair[8:])), SIDE)
    total = one
    for s in range(1, n):
        total = total + hop_row(one, s, n)
    for flip in (1, 2):
        total = total + hop_dp(total, flip)

    return (
        result[:length].astype(BF16)[None],
        grad_stream[:length].astype(BF16)[None],
        total[0],
        total[1],
        ga[:, :part].astype(F32),
        total[6, :part],
        ga[:, part : 2 * part].astype(F32),
        ga[:, 2 * part : 3 * part].astype(F32),
        total[6, 2 * part : 3 * part],
        ga[:, 3 * part :].astype(F32).T,
        total[2],
        total[3],
        total[4],
        ge[:, :ff_part].astype(F32),
        total[7, :ff_part],
        gs[:, :ff_part].astype(F32).T,
        total[5],
    )


def solution(mesh):
    batch = P(("dp", "row", "col"), None, None)
    into, out, cols, whole = P("row", "col"), P("col", "row"), P("col"), P()
    return jax.shard_map(
        functools.partial(layer, mesh.shape["row"]),
        mesh=mesh,
        in_specs=(batch, batch, whole, whole, into, cols, into, into, cols, out, whole, whole, whole, into, cols, out, whole),
        out_specs=(batch, batch, whole, whole, into, cols, into, into, cols, out, whole, whole, whole, into, cols, out, whole),
        check_vma=False,
    )
```

```python
import functools, math
import jax
import jax.numpy as jnp
from jax import lax
from jax.experimental import pallas as pl
from jax.experimental.pallas import tpu as pltpu
from jax.sharding import PartitionSpec as P

HEAD = 72
LANE = 128
F32, BF16 = jnp.float32, jnp.bfloat16
NT = (((1,), (1,)), ((), ()))
TN = (((0,), (0,)), ((), ()))
ANY = pl.BlockSpec(memory_space=pl.ANY)
VM = pl.BlockSpec(memory_space=pltpu.VMEM)
VLIM = 60 * 1024 * 1024


def dot(a, b):
    return jnp.dot(a, b, preferred_element_type=F32)


def dot_nt(a, b):
    return lax.dot_general(a, b, NT, preferred_element_type=F32)


def dot_tn(a, b):
    return lax.dot_general(a, b, TN, preferred_element_type=F32)


def tiles(total, width, body):
    count = -(-total // width)

    def step(i, _):
        body(pl.multiple_of(jnp.minimum(i * width, total - width), LANE))
        return 0

    lax.fori_loop(0, count, step, 0)


class Copies:
    def __init__(self, sems):
        self.sems, self.n = sems, 0

    def __call__(self, src, dst):
        copy = pltpu.make_async_copy(src, dst, self.sems.at[self.n])
        self.n += 1
        copy.start()
        return copy


def load_rows(copies, blocks, dst):
    n = len(blocks)
    size = dst.shape[0] // n
    me = lax.axis_index("row")
    out = []
    for s, block in enumerate(blocks):
        at = lax.rem(me - s + n, n) * size
        for piece in block if isinstance(block, (list, tuple)) else (block,):
            out.append(copies(piece, dst.at[pl.ds(pl.multiple_of(at, 8), piece.shape[0]), :]))
            at += piece.shape[0]
    return out


def nested(refs, shape):
    return jax.tree.unflatten(shape, refs)


def wait(copies):
    for copy in copies:
        copy.wait()


GC = math.sqrt(2.0 / math.pi)


def ff_kernel(shape, *refs):
    n = shape.num_leaves
    in2, cot, bias = refs[:3]
    eb, sb = nested(refs[3 : 3 + n], shape)
    res_in, gi_in = refs[3 + n : 5 + n]
    hid_o, gb_o, res_o, gi_o, db = refs[5 + n : 10 + n]
    in2_v, cot_v, e_v, s_v, hid_v, gb_v, res_v, gi_v, sems = refs[10 + n :]
    c = Copies(sems)
    first = [c(in2, in2_v)] + load_rows(c, eb, e_v)
    second = [c(cot, cot_v)] + load_rows(c, sb, s_v)
    third = [c(res_in, res_v), c(gi_in, gi_v)]
    wait(first)
    wait(second)
    width = e_v.shape[1]

    def hidden_tile(at):
        cols = pl.ds(at, 256)
        b = dot(in2_v[...], e_v[:, cols]) + bias[1:2, cols]
        sq = b * b
        t = jnp.tanh(GC * b * (1.0 + 0.044715 * sq))
        half = 0.5 * (1.0 + t)
        hid_v[:, cols] = (b * half).astype(BF16)
        slope = half + (0.5 * GC) * b * (1.0 - t * t) * (1.0 + (3 * 0.044715) * sq)
        g = dot(cot_v[...], s_v[:, cols]) * slope
        gb_v[:, cols] = g.astype(BF16)
        db[:, cols] = jnp.sum(g, axis=0, keepdims=True)

    tiles(width, 256, hidden_tile)
    out = [c(hid_v, hid_o), c(gb_v, gb_o)]
    wait(third)

    for a in range(0, width, 256):
        w = min(256, width - a)
        res_v[:, a : a + w] += dot_nt(hid_v[...], s_v[a : a + w, :])
        gi_v[:, a : a + w] += dot_nt(gb_v[...], e_v[a : a + w, :])
    out += [c(res_v, res_o), c(gi_v, gi_o)]
    wait(out)


def ff(in2, cot, bias, eb, sb, res, gi):
    blocks, shape = jax.tree.flatten((eb, sb))
    n, (t, d) = len(blocks), in2.shape
    w = blocks[0].shape[1]
    o = jax.ShapeDtypeStruct
    return pl.pallas_call(
        functools.partial(ff_kernel, shape),
        name="ff",
        in_specs=[ANY, ANY, VM] + [ANY] * (n + 2),
        out_specs=[ANY] * 4 + [VM],
        out_shape=[o((t, w), BF16), o((t, w), BF16), o((t, d), F32), o((t, d), F32), o((1, w), F32)],
        scratch_shapes=[
            pltpu.VMEM((t, d), BF16), pltpu.VMEM((t, d), BF16),
            pltpu.VMEM((d, w), BF16), pltpu.VMEM((d, w), BF16),
            pltpu.VMEM((t, w), BF16), pltpu.VMEM((t, w), BF16),
            pltpu.VMEM((t, d), F32), pltpu.VMEM((t, d), F32),
            pltpu.SemaphoreType.DMA((n + 8,)),
        ],
        input_output_aliases={3 + n: 2, 4 + n: 3},
        compiler_params=pltpu.CompilerParams(vmem_limit_bytes=VLIM),
        cost_estimate=pl.CostEstimate(flops=8 * t * d * w, bytes_accessed=4 * d * w + 12 * t * d + 8 * t * d, transcendentals=t * w),
    )(in2, cot, bias, *blocks, res, gi)


def lanes(shape):
    return lax.broadcasted_iota(jnp.int32, shape, 1)


def pick(ref, at):
    base = at // LANE * LANE
    window = ref[:, base : base + 2 * LANE]
    shift = at - base
    if shift:
        window = pltpu.roll(window, 2 * LANE - shift, 1)
    return window[:, :LANE]


def put(ref, at, value):
    base = min(at // LANE * LANE, ref.shape[1] - 2 * LANE)
    wide = jnp.concatenate((value, jnp.zeros_like(value)), axis=1)
    if at - base:
        wide = pltpu.roll(wide, at - base, 1)
    ref[:, base : base + 2 * LANE] += wide


def split3(value):
    hi = value.astype(BF16).astype(F32)
    rest = value - hi
    mid = rest.astype(BF16).astype(F32)
    return hi, mid, rest - mid


SCALE = HEAD ** -0.5
C2 = SCALE * math.log2(math.e)
PENALTY = -1e30


def attn_kernel(shape, heads, length, chunk, *refs):
    n = shape.num_leaves
    in1, bias = refs[:2]
    ab = nested(refs[2 : 2 + n], shape)
    mid_in = refs[2 + n]
    q_o, k_o, v_o, att_o, mid_o = refs[3 + n : 8 + n]
    in1_v, a_v, qkv_v, q_v, k_v, v_v, o_v, att_v, mid_v, attb_v, sems = refs[8 + n :]
    t = in1_v.shape[0]
    c = Copies(sems)
    first = [c(in1, in1_v)] + load_rows(c, ab, a_v)
    third = [c(mid_in, mid_v)]
    wait(first)

    def proj(at):
        cols = pl.ds(at, 256)
        qkv_v[:, cols] = dot(in1_v[...], a_v[:, cols]) + bias[0:1, cols]

    tiles(7 * LANE, 256, proj)
    lane = lanes((t, LANE))
    row = lax.broadcasted_iota(jnp.int32, (t, LANE), 0)
    tail_k = jnp.where(lane < HEAD + 3, 1.0, jnp.where((lane == HEAD + 3) & (row >= length), 1.0, 0.0))
    tail_q = jnp.where(lane == HEAD + 3, PENALTY, 0.0)
    tail_v = jnp.where(lane < HEAD + 2, 1.0, 0.0)
    part = HEAD * heads
    for j in range(heads):
        q_v[j] = jnp.where(lane < HEAD, pick(qkv_v, HEAD * j), tail_q).astype(BF16)
        k_v[j] = jnp.where(lane < HEAD, pick(qkv_v, part + HEAD * j), tail_k).astype(BF16)
        v_v[j] = jnp.where(lane < HEAD, pick(qkv_v, 2 * part + HEAD * j), tail_v).astype(BF16)
    out = [c(k_v, k_o), c(v_v, v_o)]

    def head(j, _):
        def rows(i, _):
            at = pl.ds(pl.multiple_of(i * chunk, 16), chunk)
            q = q_v[j, at, :]
            s = dot_nt(q, k_v[j])
            m = jnp.max(s, axis=1, keepdims=True)
            p = jnp.exp2((s - m) * C2)
            o = dot(p.astype(BF16), v_v[j])
            ln = lanes((chunk, LANE))
            total = jnp.sum(jnp.where(ln == HEAD, o, 0.0), axis=1, keepdims=True)
            o_v[j, at, :] = jnp.where(ln < HEAD, o / total, 0.0)
            hi, mid, lo = split3(m + jnp.log2(total) * (1.0 / C2))
            aug = jnp.where(ln == HEAD, -hi, jnp.where(ln == HEAD + 1, -mid, jnp.where(ln == HEAD + 2, -lo, q.astype(F32))))
            q_v[j, at, :] = aug.astype(BF16)
            return 0

        return lax.fori_loop(0, t // chunk, rows, 0)

    lax.fori_loop(0, heads, head, 0)
    out += [c(q_v, q_o)]
    att_v[...] = jnp.zeros_like(att_v)
    for j in range(heads):
        put(att_v, 3 * LANE - part + HEAD * j, o_v[j])
    attb_v[...] = att_v[...].astype(BF16)
    out += [c(attb_v, att_o)]
    wait(third)
    d = mid_v.shape[1]
    for a in range(0, d, 256):
        w = min(256, d - a)
        mid_v[:, a : a + w] += dot_nt(attb_v[...], a_v[a : a + w, 6 * LANE : 9 * LANE])
    out += [c(mid_v, mid_o)]
    wait(out)


def attn(in1, bias, ab, mid, length, chunk=368):
    blocks, shape = jax.tree.flatten(ab)
    n, (t, d) = len(blocks), in1.shape
    w = blocks[0].shape[1]
    heads = w // 4 // HEAD
    o = jax.ShapeDtypeStruct
    hs = (heads, t, LANE)
    return pl.pallas_call(
        functools.partial(attn_kernel, shape, heads, length, chunk),
        name="attn",
        in_specs=[ANY, VM] + [ANY] * (n + 1),
        out_specs=[ANY] * 5,
        out_shape=[o(hs, BF16)] * 3 + [o((t, 3 * LANE), BF16), o((t, d), F32)],
        scratch_shapes=[
            pltpu.VMEM((t, d), BF16), pltpu.VMEM((d, w), BF16), pltpu.VMEM((t, 8 * LANE), F32),
            pltpu.VMEM(hs, BF16), pltpu.VMEM(hs, BF16), pltpu.VMEM(hs, BF16), pltpu.VMEM(hs, F32),
            pltpu.VMEM((t, 3 * LANE), F32), pltpu.VMEM((t, d), F32), pltpu.VMEM((t, 3 * LANE), BF16),
            pltpu.SemaphoreType.DMA((n + 8,)),
        ],
        input_output_aliases={2 + n: 4},
        compiler_params=pltpu.CompilerParams(vmem_limit_bytes=VLIM),
        cost_estimate=pl.CostEstimate(flops=2 * t * d * w + 8 * heads * t * t * LANE, bytes_accessed=2 * d * w + 10 * t * d, transcendentals=heads * t * t),
    )(in1, bias, *blocks, mid)


def back_kernel(shape, heads, chunk, *refs):
    n = shape.num_leaves
    gm = refs[0]
    ab = nested(refs[1 : 1 + n], shape)
    q_i, k_i, v_i, att_i, gi_in = refs[1 + n : 6 + n]
    dqkv_o, gi_o, db = refs[6 + n : 9 + n]
    gm_v, a_v, ga_v, q_v, k_v, v_v, g_v, att_v, ds_v, dq_v, dk_v, dv_v, pack_v, packb_v, gi_v, sems = refs[9 + n :]
    t = gm_v.shape[0]
    c = Copies(sems)
    first = [c(gm, gm_v)] + load_rows(c, ab, a_v)
    second = [c(att_i, att_v), c(q_i, q_v), c(k_i, k_v), c(v_i, v_v)]
    third = [c(gi_in, gi_v)]
    wait(first)
    ga_v[...] = dot(gm_v[...], a_v[:, 6 * LANE : 9 * LANE])
    lane = lanes((t, LANE))
    part = HEAD * heads
    wait(second)
    att = pack_v.at[:, : 3 * LANE]
    att[...] = att_v[...].astype(F32)
    for j in range(heads):
        at = 3 * LANE - part + HEAD * j
        base = min(at // LANE * LANE, LANE)

        def grab(ref):
            window = ref[:, base : base + 2 * LANE]
            return pltpu.roll(window, 2 * LANE - (at - base), 1)[:, :LANE] if at > base else window[:, :LANE]

        g = jnp.where(lane < HEAD, grab(ga_v), 0.0).astype(BF16).astype(F32)
        delta = jnp.sum(g * grab(att), axis=1, keepdims=True)
        hi = delta.astype(BF16).astype(F32)
        g_v[j] = jnp.where(lane == HEAD, -hi, jnp.where(lane == HEAD + 1, hi - delta, g)).astype(BF16)

    def head(j, _):
        def rows(i, _):
            at = pl.ds(pl.multiple_of(i * chunk, 16), chunk)
            p = jnp.exp2(dot_nt(k_v[j, at, :], q_v[j]) * C2)
            pb = p.astype(BF16)
            ds = (p * dot_nt(v_v[j, at, :], g_v[j])).astype(BF16)
            dv_v[j, at, :] = dot(pb, g_v[j])
            dk_v[j, at, :] = dot(ds, q_v[j]) * SCALE
            ds_v[at, :] = ds
            return 0

        lax.fori_loop(0, t // chunk, rows, 0)
        dq_v[j] = dot_tn(ds_v[...], k_v[j]) * SCALE
        return 0

    lax.fori_loop(0, heads, head, 0)
    pack_v[...] = jnp.zeros_like(pack_v)
    for j in range(heads):
        put(pack_v, HEAD * j, jnp.where(lane < HEAD, dq_v[j], 0.0))
        put(pack_v, part + HEAD * j, jnp.where(lane < HEAD, dk_v[j], 0.0))
        put(pack_v, 2 * part + HEAD * j, jnp.where(lane < HEAD, dv_v[j], 0.0))
    db[...] = jnp.sum(pack_v[...], axis=0, keepdims=True)
    packb_v[...] = pack_v[...].astype(BF16)
    out = [c(packb_v, dqkv_o)]
    wait(third)
    d = gi_v.shape[1]
    for a in range(0, d, 256):
        w = min(256, d - a)
        gi_v[:, a : a + w] += dot_nt(packb_v[...], a_v[a : a + w, : 7 * LANE])
    out += [c(gi_v, gi_o)]
    wait(out)


def back(gm, ab, q, k, v, att, gi, chunk=368):
    blocks, shape = jax.tree.flatten(ab)
    n, (t, d) = len(blocks), gm.shape
    w = blocks[0].shape[1]
    heads = q.shape[0]
    o = jax.ShapeDtypeStruct
    hs = (heads, t, LANE)
    return pl.pallas_call(
        functools.partial(back_kernel, shape, heads, chunk),
        name="back",
        in_specs=[ANY] * (n + 6),
        out_specs=[ANY] * 2 + [VM],
        out_shape=[o((t, 7 * LANE), BF16), o((t, d), F32), o((1, 7 * LANE), F32)],
        scratch_shapes=[
            pltpu.VMEM((t, d), BF16), pltpu.VMEM((d, w), BF16), pltpu.VMEM((t, 3 * LANE), F32),
            pltpu.VMEM(hs, BF16), pltpu.VMEM(hs, BF16), pltpu.VMEM(hs, BF16), pltpu.VMEM(hs, BF16),
            pltpu.VMEM((t, 3 * LANE), BF16), pltpu.VMEM((t, t), BF16),
            pltpu.VMEM(hs, F32), pltpu.VMEM(hs, F32), pltpu.VMEM(hs, F32),
            pltpu.VMEM((t, 7 * LANE), F32), pltpu.VMEM((t, 7 * LANE), BF16), pltpu.VMEM((t, d), F32),
            pltpu.SemaphoreType.DMA((n + 8,)),
        ],
        input_output_aliases={5 + n: 1},
        compiler_params=pltpu.CompilerParams(vmem_limit_bytes=VLIM),
        cost_estimate=pl.CostEstimate(flops=2 * t * d * w + 20 * heads * t * t * LANE, bytes_accessed=2 * d * w + 16 * t * d, transcendentals=heads * t * t),
    )(gm, *blocks, q, k, v, att, gi)


def grads_kernel(n, groups, *refs):
    k = len(groups)
    ins = refs[: 4 * k]
    outs = refs[4 * k : 4 * k + n]
    scratch = refs[4 * k + n :]
    lhs, rhs = scratch[: 2 * k], scratch[2 * k : 4 * k]
    acc, tile_v, sems, osem = scratch[4 * k :]
    c = Copies(sems)
    cps = []
    for i in range(k):
        cps += [c(ins[4 * i + u], (lhs if u < 2 else rhs)[2 * i + u % 2]) for u in range(4)]
    wait(cps)
    size = outs[0].shape[0]
    t = rhs[0].shape[0]
    me = lax.axis_index("row")

    def step(s, _):
        slot = lax.rem(s, 2)
        row = pl.multiple_of(lax.rem(me + s, n) * size, 16)
        rows = pl.ds(row, size)

        @pl.when(s >= 2)
        def _():
            pltpu.make_async_copy(tile_v.at[slot], outs[0], osem.at[slot]).wait()

        if k == 1:
            def body(at):
                cols = pl.ds(at, 256)
                tile_v[slot, :, cols] = (
                    dot(lhs[0][rows, :t], rhs[0][:, cols]) + dot(lhs[1][rows, :t], rhs[1][:, cols])
                ).astype(BF16)

            tiles(groups[0][1], 256, body)
        else:
            for i, (start, width) in enumerate(groups):
                done = 0 if i == 0 else groups[i - 1][0] + groups[i - 1][1]
                for a in range(0, width, 256):
                    w = min(256, width - a)
                    value = dot(lhs[2 * i][rows, :t], rhs[2 * i][:, a : a + w]) + dot(
                        lhs[2 * i + 1][rows, :t], rhs[2 * i + 1][:, a : a + w]
                    )
                    at = start + a
                    if at < done:
                        o = done - at
                        value = jnp.concatenate((value[:, :o] + acc[:, at : at + o], value[:, o:]), axis=1) if o < w else value + acc[:, at : at + w]
                    acc[:, at : at + w] = value
            tile_v[slot] = acc[...].astype(BF16)
        for u in range(n):
            @pl.when(s == u)
            def _():
                pltpu.make_async_copy(tile_v.at[slot], outs[u], osem.at[slot]).start()
        return 0

    lax.fori_loop(0, n, step, 0)
    for u in range(max(0, n - 2), n):
        pltpu.make_async_copy(tile_v.at[u % 2], outs[u], osem.at[u % 2]).wait()


def grads(n, terms, width):
    k = len(terms)
    groups = tuple((term[0], term[3].shape[1]) for term in terms)
    flat = [array for term in terms for array in term[1:]]
    d, t = terms[0][1].shape[0], terms[0][3].shape[0]
    size = d // n
    scratch = [pltpu.VMEM(term[1].shape, BF16) for term in terms for _ in range(2)]
    scratch += [pltpu.VMEM(term[3].shape, BF16) for term in terms for _ in range(2)]
    flops = sum(4 * d * t * w for _, w in groups)
    return pl.pallas_call(
        functools.partial(grads_kernel, n, groups),
        name="grads",
        in_specs=[ANY] * (4 * k),
        out_specs=[ANY] * n,
        out_shape=[jax.ShapeDtypeStruct((size, width), BF16)] * n,
        scratch_shapes=scratch + [
            pltpu.VMEM((size, width if k > 1 else LANE), F32), pltpu.VMEM((2, size, width), BF16),
            pltpu.SemaphoreType.DMA((4 * k,)), pltpu.SemaphoreType.DMA((2,)),
        ],
        compiler_params=pltpu.CompilerParams(vmem_limit_bytes=VLIM),
        cost_estimate=pl.CostEstimate(flops=flops, bytes_accessed=2 * d * width + 8 * t * d, transcendentals=0),
    )(*flat)


EPS = 1e-6
ROWS = 16


def row_loop(count, body, init):
    return lax.fori_loop(0, count // ROWS, lambda i, carry: body(pl.ds(pl.multiple_of(i * ROWS, ROWS), ROWS), carry), init, unroll=2 if count // ROWS % 2 == 0 else 3 if count // ROWS % 3 == 0 else 1)


def stats(x):
    average = jnp.mean(x, axis=-1, keepdims=True)
    second = jnp.mean(x * x, axis=-1, keepdims=True)
    return average, lax.rsqrt(second - average * average + EPS)


def turn(dst, src):
    if dst.shape[1] > src.shape[0]:
        dst[...] = jnp.zeros_like(dst)
    for a in range(0, src.shape[1], LANE):
        w = min(LANE, src.shape[1] - a)
        dst[a : a + w, : src.shape[0]] = src[:, a : a + w].T


def fold(x):
    return jnp.sum(x.reshape(x.shape[0] // 8, 8, x.shape[1]), axis=0)


def weave_kernel(q, k, v, o, out, all_v):
    part = q.shape[0]
    for i, ref in enumerate((q, k, v, o)):
        all_v[i * part : (i + 1) * part, :] = ref[...]
    turn(out, all_v)


def weave(q, k, v, o):
    part, size = q.shape
    return pl.pallas_call(
        weave_kernel,
        name="weave",
        in_specs=[VM] * 4,
        out_specs=VM,
        out_shape=jax.ShapeDtypeStruct((size, 4 * part), BF16),
        scratch_shapes=[pltpu.VMEM((4 * part, size), BF16)],
    )(q, k, v, o)


def unweave_kernel(mine, theirs, q, k, v, o):
    part = q.shape[0]
    even = lax.rem(lax.axis_index("dp"), 2) == 0
    for a in range(0, 4 * part, LANE):
        first = jnp.where(even, mine[:, a : a + LANE], theirs[:, a : a + LANE])
        last = jnp.where(even, theirs[:, a : a + LANE], mine[:, a : a + LANE])
        both = jnp.concatenate((first, last)).astype(F32).T
        for i, ref in enumerate((q, k, v, o)):
            lo, hi = max(a, i * part), min(a + LANE, (i + 1) * part)
            if lo < hi:
                ref[lo - i * part : hi - i * part, :] = both[lo - a : hi - a, :]


def unweave(mine, theirs, part):
    size = 2 * mine.shape[0]
    return pl.pallas_call(
        unweave_kernel,
        name="unweave",
        in_specs=[VM] * 2,
        out_specs=[VM] * 4,
        out_shape=[jax.ShapeDtypeStruct((part, size), F32)] * 4,
        compiler_params=pltpu.CompilerParams(vmem_limit_bytes=VLIM),
    )(mine, theirs)


def enter_kernel(x, cot, gain, shift, bias, in1, in1_t, cot_p, cot_t, mid):
    length, t = x.shape[0], in1.shape[0]
    whole = length // ROWS * ROWS

    def rows(at, value):
        value = value.astype(F32)
        average, inverse = stats(value)
        in1[at, :] = ((value - average) * inverse * gain[...] + shift[...]).astype(BF16)
        mid[at, :] = value + bias[...]

    def step(at, _):
        rows(at, x[at, :])
        cot_p[at, :] = cot[at, :]
        return 0

    row_loop(whole, step, 0)
    if whole < t:
        last = pl.ds(whole, ROWS)
        pad = jnp.zeros((t - length, x.shape[1]), F32)
        rows(last, jnp.concatenate((x[whole:length, :].astype(F32), pad)))
        cot_p[last, :] = jnp.concatenate((cot[whole:length, :].astype(F32), pad)).astype(BF16)
    turn(in1_t, in1)
    turn(cot_t, cot_p)


def enter(x, cot, gain, shift, bias, t):
    d = x.shape[1]
    tp = -(-t // LANE) * LANE
    o = jax.ShapeDtypeStruct
    return pl.pallas_call(
        enter_kernel,
        name="enter",
        in_specs=[VM] * 5,
        out_specs=[VM] * 5,
        out_shape=[o((t, d), BF16), o((d, tp), BF16), o((t, d), BF16), o((d, tp), BF16), o((t, d), F32)],
        compiler_params=pltpu.CompilerParams(vmem_limit_bytes=VLIM),
    )(x, cot, gain, shift, bias)


def middle_kernel(mid, gain, shift, bias, in2, in2_t, res):
    def step(at, _):
        value = mid[at, :]
        average, inverse = stats(value)
        in2[at, :] = ((value - average) * inverse * gain[...] + shift[...]).astype(BF16)
        res[at, :] = value + bias[...]
        return 0

    row_loop(mid.shape[0], step, 0)
    turn(in2_t, in2)


def middle_norm(mid, gain, shift, bias):
    t, d = mid.shape
    tp = -(-t // LANE) * LANE
    o = jax.ShapeDtypeStruct
    return pl.pallas_call(
        middle_kernel,
        name="middle",
        in_specs=[VM] * 4,
        out_specs=[VM] * 3,
        out_shape=[o((t, d), BF16), o((d, tp), BF16), o((t, d), F32)],
        compiler_params=pltpu.CompilerParams(vmem_limit_bytes=VLIM),
    )(mid, gain, shift, bias)


def back_row(x, grad, gain):
    average, inverse = stats(x)
    normed = (x - average) * inverse
    scaled = grad * gain
    first = jnp.mean(scaled, axis=-1, keepdims=True)
    second = jnp.mean(scaled * normed, axis=-1, keepdims=True)
    return inverse * (scaled - first - normed * second), grad * normed


def turn_back_kernel(grad2, mid, cot, gain, gm32, gm, gm_t, sums):
    d = mid.shape[1]
    zero = jnp.zeros((8, d), F32)

    def step(at, carry):
        g, c = grad2[at, :], cot[at, :].astype(F32)
        inner, product = back_row(mid[at, :], g, gain[...])
        total = c + inner
        gm32[at, :] = total
        gm[at, :] = total.astype(BF16)
        return tuple(a + fold(b) for a, b in zip(carry, (total, product, g, c)))

    carry = row_loop(mid.shape[0], step, (zero,) * 4)
    for i, value in enumerate(carry):
        sums[i : i + 1, :] = jnp.sum(value, axis=0, keepdims=True)
    turn(gm_t, gm)


def turn_back(grad2, mid, cot, gain):
    t, d = mid.shape
    tp = -(-t // LANE) * LANE
    o = jax.ShapeDtypeStruct
    return pl.pallas_call(
        turn_back_kernel,
        name="turnback",
        in_specs=[VM] * 4,
        out_specs=[VM] * 4,
        out_shape=[o((t, d), F32), o((t, d), BF16), o((d, tp), BF16), o((4, d), F32)],
        compiler_params=pltpu.CompilerParams(vmem_limit_bytes=VLIM),
    )(grad2, mid, cot, gain)


def leave_kernel(grad1, x, gm32, gain, out, sums):
    length, d = x.shape
    t = grad1.shape[0]
    whole = length // ROWS * ROWS
    zero = jnp.zeros((8, d), F32)

    def rows(at, value, carry):
        g = grad1[at, :]
        inner, product = back_row(value, g, gain[...])
        return gm32[at, :] + inner, tuple(a + fold(b) for a, b in zip(carry, (product, g)))

    def step(at, carry):
        total, carry = rows(at, x[at, :].astype(F32), carry)
        out[at, :] = total.astype(BF16)
        return carry

    carry = row_loop(whole, step, (zero,) * 2)
    if whole < t:
        pad = jnp.zeros((t - length, d), F32)
        total, carry = rows(pl.ds(whole, ROWS), jnp.concatenate((x[whole:length, :].astype(F32), pad)), carry)
        out[whole:length, :] = total[: length - whole, :].astype(BF16)
    for i, value in enumerate(carry):
        sums[i : i + 1, :] = jnp.sum(value, axis=0, keepdims=True)


def leave(grad1, x, gm32, gain):
    o = jax.ShapeDtypeStruct
    return pl.pallas_call(
        leave_kernel,
        name="leave",
        in_specs=[VM] * 4,
        out_specs=[VM] * 2,
        out_shape=[o(x.shape, BF16), o((2, x.shape[1]), F32)],
        compiler_params=pltpu.CompilerParams(vmem_limit_bytes=VLIM),
    )(grad1, x, gm32, gain)


CORE, SIDE = 1, 2


def hop_row(value, shift, size):
    return lax.ppermute(value, "row", [(i, (i + shift) % size) for i in range(size)])


def hop_col(value, flip):
    return lax.ppermute(value, "col", [(i, i ^ flip) for i in range(4)])


def hop_dp(value, flip):
    return lax.ppermute(value, "dp", [(i, i ^ flip) for i in range(4)])


def after(value, *first):
    return lax.optimization_barrier((value, *first))[0]


def near(block, n):
    return [block] + [hop_row(block, s, n) for s in range(1, n)], hop_col(block, SIDE)


def diagonal(own, side, n, via):
    parts = [side]
    half = side.shape[0] // 2
    for s in range(1, n):
        if via == "row":
            parts.append(hop_row(side, s, n))
        elif via == "col":
            parts.append(hop_col(own[s], SIDE))
        else:
            parts.append((hop_row(side[:half], s, n), hop_col(own[s][half:], SIDE)))
    return parts


def across(parts):
    return [jax.tree.map(lambda b: hop_col(b, CORE), part) for part in parts]


def add(a, b):
    return (a.astype(F32) + b.astype(F32)).astype(BF16)


def over_row(parts, n):
    total = parts[0]
    for s in range(1, n):
        total = add(total, hop_row(parts[s], s, n))
    return total


def over_dp(total):
    half = total.shape[0] // 2
    low = lax.rem(lax.axis_index("dp"), 2)
    mine = lax.dynamic_slice_in_dim(total, low * half, half, 0)
    theirs = lax.dynamic_slice_in_dim(total, (1 - low) * half, half, 0)
    mine = add(mine, hop_dp(theirs, 1))
    mine = add(mine, hop_dp(mine, 2))
    return mine, hop_dp(mine, 1)


def joined_halves(mine, theirs):
    even = lax.rem(lax.axis_index("dp"), 2) == 0
    return jnp.where(even, jnp.concatenate((mine, theirs)), jnp.concatenate((theirs, mine))).astype(F32)


def layer(n, images, cotangent, first_gain, first_shift, query_weight, query_bias, key_weight, value_weight, value_bias,
          output_weight, output_bias, second_gain, second_shift, expand_weight, expand_bias, shrink_weight, shrink_bias):
    length, d = images.shape[1:]
    t = -(-length // 16) * 16
    part, ff_part = query_weight.shape[1], expand_weight.shape[1]
    wide = 4 * part
    pad_ff = ((0, 0), (0, wide - ff_part))
    a_own = weave(query_weight.T, key_weight.T, value_weight.T, output_weight)
    zeros = jnp.zeros((part,), F32)
    bias_own = jnp.stack((jnp.concatenate((query_bias, zeros, value_bias, zeros)), jnp.pad(expand_bias, pad_ff[1:])))
    a_near, a_side = near(a_own, n)
    bias_side = hop_col(bias_own, SIDE)
    biases = [bias_own, bias_side, hop_col(bias_own, CORE), hop_col(bias_side, CORE)]
    row = lambda v: v.reshape(1, -1)
    images, cotangent = images[0], cotangent[0]
    input1, in1_t, cot, cot_t, middle = enter(
        after(images, a_own), cotangent, row(first_gain), row(first_shift), row(output_bias), t)
    e_own = jnp.pad(expand_weight, pad_ff)
    s_own = jnp.pad(shrink_weight.T, pad_ff)

    a_far = diagonal(a_near, a_side, n, "both")
    a_all = [a_near, a_far, across(a_near), across(a_far)]
    e_near, e_side = near(after(e_own, a_side), n)
    s_near, s_side = near(after(s_own, a_side), n)
    e_far = diagonal(e_near, e_side, n, "row")
    s_far = diagonal(s_near, s_side, n, "col")
    e_all = [e_near, e_far, across(e_near), across(e_far)]
    s_all = [s_near, s_far, across(s_near), across(s_far)]
    cot_t2 = hop_col(after(cot_t, a_side), CORE)
    in1_t2 = hop_col(after(in1_t, a_side), CORE)

    kept = {}
    last = middle
    for slot in (0, 2, 1, 3):
        *kept[slot], middle = attn(input1, after(biases[slot], last), a_all[slot], middle, length)
        last = kept[slot][3]
    input2, in2_t, result = middle_norm(middle, row(second_gain), row(second_shift), row(shrink_bias))
    in2_t2 = hop_col(in2_t, CORE)
    att2 = [hop_col(kept[s + 2][3], CORE) for s in (0, 1)]
    grad2 = jnp.zeros((t, d), F32)
    hidden, before, expand_sums, ge, gs = {}, {}, {}, {}, {}

    def feed(slot, last, result, grad2):
        hidden[slot], before[slot], result, grad2, expand_sums[slot] = ff(
            input2, cot, after(biases[slot], last), e_all[slot], s_all[slot], result, grad2)
        return result, grad2

    def expand_grads(slot, last):
        other = hop_col(before[slot + 2], CORE)
        ge[slot] = grads(n, [(0, in2_t, in2_t2, after(before[slot], last), other)], wide)
        return ge[slot][-1]

    def shrink_grads(slot, last):
        other = hop_col(hidden[slot + 2], CORE)
        gs[slot] = grads(n, [(0, cot_t, cot_t2, after(hidden[slot], last), other)], wide)
        return gs[slot][-1]

    result, grad2 = feed(0, in2_t, result, grad2)
    result, grad2 = feed(2, expand_sums[0], result, grad2)
    result, grad2 = feed(1, expand_sums[2], result, grad2)
    last = expand_grads(0, expand_sums[1])
    result, grad2 = feed(3, last, result, grad2)
    last = shrink_grads(0, expand_sums[3])
    last = shrink_grads(1, last)
    last = expand_grads(1, last)
    gm32, gm, gm_t, middle_sums = turn_back(grad2, middle, cot, after(row(second_gain), last))
    gm_t2 = hop_col(gm_t, CORE)
    grad1 = jnp.zeros((t, d), F32)
    joined, joined_sums, ga = {}, {}, {}

    def attend_back(slot, last, grad1):
        q, k, v, att = kept[slot]
        joined[slot], grad1, joined_sums[slot] = back(gm, a_all[slot], q, k, v, after(att, last), grad1)
        return grad1

    def joined_grads(slot, last):
        other = hop_col(joined[slot + 2], CORE)
        ga[slot] = grads(n, [
            (0, in1_t, in1_t2, after(joined[slot], last), other),
            (wide - 384, gm_t, gm_t2, kept[slot][3], att2[slot]),
        ], wide)
        return ga[slot][-1]

    grad1 = attend_back(3, middle_sums, grad1)
    grad1 = attend_back(1, joined_sums[3], grad1)
    grad1 = attend_back(2, joined_sums[1], grad1)
    last = joined_grads(1, joined_sums[2])
    grad1 = attend_back(0, last, grad1)
    last = joined_grads(0, joined_sums[0])

    e_total = over_dp(add(over_row(ge[0], n), hop_col(over_row(ge[1], n), SIDE)))
    s_total = over_dp(over_row([add(a, hop_col(b, SIDE)) for a, b in zip(gs[0], gs[1])], n))
    a_total = over_dp(add(over_row(ga[0], n), hop_col(over_row(ga[1], n), SIDE)))
    grad_stream, first_sums = leave(grad1, images, gm32, after(row(first_gain), last))

    sums = {s: jnp.concatenate((jnp.pad(joined_sums[s], ((0, 0), (0, wide - joined_sums[s].shape[1]))), expand_sums[s])) for s in range(4)}
    features = jnp.concatenate((first_sums, middle_sums))
    pair = jnp.concatenate((features, sums[0], sums[1])) + hop_col(jnp.concatenate((features, sums[2], sums[3])), CORE)
    one = pair[:8] + hop_col(jnp.concatenate((pair[:6], pair[8:])), SIDE)
    total = one
    for s in range(1, n):
        total = total + hop_row(one, s, n)
    for flip in (1, 2):
        total = total + hop_dp(total, flip)
    gq, gk, gv, go = unweave(*a_total, part)
    return (
        result[:length].astype(BF16)[None],
        grad_stream[None],
        total[0],
        total[1],
        gq.T,
        total[6, :part],
        gk.T,
        gv.T,
        total[6, 2 * part : 3 * part],
        go,
        total[2],
        total[3],
        total[4],
        joined_halves(*e_total)[:, :ff_part],
        total[7, :ff_part],
        joined_halves(*s_total)[:, :ff_part].T,
        total[5],
    )


def solution(mesh):
    batch = P(("dp", "row", "col"), None, None)
    into, out, cols, whole = P("row", "col"), P("col", "row"), P("col"), P()

    def step(*args):
        return layer(mesh.shape["row"], *args)

    return jax.shard_map(
        step,
        mesh=mesh,
        in_specs=(batch, batch, whole, whole, into, cols, into, into, cols, out, whole, whole, whole, into, cols, out, whole),
        out_specs=(batch, batch, whole, whole, into, cols, into, into, cols, out, whole, whole, whole, into, cols, out, whole),
        check_vma=False,
    )
```

```python
import functools, math
import jax
import jax.numpy as jnp
from jax import lax
from jax.experimental import pallas as pl
from jax.experimental.pallas import tpu as pltpu
from jax.sharding import PartitionSpec as P

HEAD = 72
LANE = 128
F32, BF16 = jnp.float32, jnp.bfloat16
NT = (((1,), (1,)), ((), ()))
TN = (((0,), (0,)), ((), ()))
ANY = pl.BlockSpec(memory_space=pl.ANY)
VM = pl.BlockSpec(memory_space=pltpu.VMEM)
VLIM = 60 * 1024 * 1024


def dot(a, b):
    return jnp.dot(a, b, preferred_element_type=F32)


def dot_nt(a, b):
    return lax.dot_general(a, b, NT, preferred_element_type=F32)


def dot_tn(a, b):
    return lax.dot_general(a, b, TN, preferred_element_type=F32)


def tiles(total, width, body):
    count = -(-total // width)

    def step(i, _):
        body(pl.multiple_of(jnp.minimum(i * width, total - width), LANE))
        return 0

    lax.fori_loop(0, count, step, 0)


class Copies:
    def __init__(self, sems):
        self.sems, self.n = sems, 0

    def __call__(self, src, dst):
        copy = pltpu.make_async_copy(src, dst, self.sems.at[self.n])
        self.n += 1
        copy.start()
        return copy


def load_rows(copies, blocks, dst):
    n = len(blocks)
    size = dst.shape[0] // n
    me = lax.axis_index("row")
    out = []
    for s, block in enumerate(blocks):
        at = lax.rem(me - s + n, n) * size
        for piece in block if isinstance(block, (list, tuple)) else (block,):
            out.append(copies(piece, dst.at[pl.ds(pl.multiple_of(at, 8), piece.shape[0]), :]))
            at += piece.shape[0]
    return out


def nested(refs, shape):
    return jax.tree.unflatten(shape, refs)


def wait(copies):
    for copy in copies:
        copy.wait()


EPS = 1e-6
ROWS = 16


def row_loop(count, body, init):
    return lax.fori_loop(0, count // ROWS, lambda i, carry: body(pl.ds(pl.multiple_of(i * ROWS, ROWS), ROWS), carry), init, unroll=2 if count // ROWS % 2 == 0 else 3 if count // ROWS % 3 == 0 else 1)


def stats(x):
    average = jnp.mean(x, axis=-1, keepdims=True)
    second = jnp.mean(x * x, axis=-1, keepdims=True)
    return average, lax.rsqrt(second - average * average + EPS)


def turn(dst, src):
    if dst.shape[1] > src.shape[0]:
        dst[...] = jnp.zeros_like(dst)
    for a in range(0, src.shape[1], LANE):
        w = min(LANE, src.shape[1] - a)
        dst[a : a + w, : src.shape[0]] = src[:, a : a + w].T


def fold(x):
    return jnp.sum(x.reshape(x.shape[0] // 8, 8, x.shape[1]), axis=0)


def weave_kernel(q, k, v, o, out, all_v):
    part = q.shape[0]
    for i, ref in enumerate((q, k, v, o)):
        all_v[i * part : (i + 1) * part, :] = ref[...]
    turn(out, all_v)


def weave(q, k, v, o):
    part, size = q.shape
    return pl.pallas_call(
        weave_kernel,
        name="weave",
        in_specs=[VM] * 4,
        out_specs=VM,
        out_shape=jax.ShapeDtypeStruct((size, 4 * part), BF16),
        scratch_shapes=[pltpu.VMEM((4 * part, size), BF16)],
    )(q, k, v, o)


def unweave_kernel(*refs):
    pieces, (q, k, v, o) = refs[:-4], refs[-4:]
    part = q.shape[0]
    even = lax.rem(lax.axis_index("dp"), 2) == 0
    for a in range(0, 4 * part, LANE):
        cols = slice(a, a + LANE)
        rows = []
        for i in range(0, len(pieces), 2):
            mine, theirs = pieces[i][:, cols].astype(F32), pieces[i + 1][:, cols].astype(F32)
            rows += [jnp.where(even, mine, theirs), jnp.where(even, theirs, mine)]
        both = jnp.concatenate(rows).T
        for i, ref in enumerate((q, k, v, o)):
            lo, hi = max(a, i * part), min(a + LANE, (i + 1) * part)
            if lo < hi:
                ref[lo - i * part : hi - i * part, :] = both[lo - a : hi - a, :]


def unweave(pieces, part):
    flat = [piece for pair in pieces for piece in pair]
    return pl.pallas_call(
        unweave_kernel,
        name="unweave",
        in_specs=[VM] * len(flat),
        out_specs=[VM] * 4,
        out_shape=[jax.ShapeDtypeStruct((part, sum(piece.shape[0] for piece in flat)), F32)] * 4,
        compiler_params=pltpu.CompilerParams(vmem_limit_bytes=VLIM),
    )(*flat)


def enter_kernel(x, cot, gain, shift, bias, in1, in1_t, cot_p, cot_t, mid):
    length, t = x.shape[0], in1.shape[0]
    whole = length // ROWS * ROWS

    def rows(at, value):
        value = value.astype(F32)
        average, inverse = stats(value)
        in1[at, :] = ((value - average) * inverse * gain[...] + shift[...]).astype(BF16)
        mid[at, :] = value + bias[...]

    def step(at, _):
        rows(at, x[at, :])
        cot_p[at, :] = cot[at, :]
        return 0

    row_loop(whole, step, 0)
    if whole < t:
        last = pl.ds(whole, ROWS)
        pad = jnp.zeros((t - length, x.shape[1]), F32)
        rows(last, jnp.concatenate((x[whole:length, :].astype(F32), pad)))
        cot_p[last, :] = jnp.concatenate((cot[whole:length, :].astype(F32), pad)).astype(BF16)
    turn(in1_t, in1)
    turn(cot_t, cot_p)


def enter(x, cot, gain, shift, bias, t):
    d = x.shape[1]
    tp = -(-t // LANE) * LANE
    o = jax.ShapeDtypeStruct
    return pl.pallas_call(
        enter_kernel,
        name="enter",
        in_specs=[VM] * 5,
        out_specs=[VM] * 5,
        out_shape=[o((t, d), BF16), o((d, tp), BF16), o((t, d), BF16), o((d, tp), BF16), o((t, d), F32)],
        compiler_params=pltpu.CompilerParams(vmem_limit_bytes=VLIM),
    )(x, cot, gain, shift, bias)


def back_row(x, grad, gain):
    average, inverse = stats(x)
    normed = (x - average) * inverse
    scaled = grad * gain
    first = jnp.mean(scaled, axis=-1, keepdims=True)
    second = jnp.mean(scaled * normed, axis=-1, keepdims=True)
    return inverse * (scaled - first - normed * second), grad * normed


def leave_body(grad1, x, gm32, gain, out, sums):
    length, d = x.shape
    t = grad1.shape[0]
    whole = length // ROWS * ROWS
    zero = jnp.zeros((8, d), F32)

    def rows(at, value, carry):
        g = grad1[at, :]
        inner, product = back_row(value, g, gain[...])
        return gm32[at, :] + inner, tuple(a + fold(b) for a, b in zip(carry, (product, g)))

    def step(at, carry):
        total, carry = rows(at, x[at, :].astype(F32), carry)
        out[at, :] = total.astype(BF16)
        return carry

    carry = row_loop(whole, step, (zero,) * 2)
    if whole < t:
        pad = jnp.zeros((t - length, d), F32)
        total, carry = rows(pl.ds(whole, ROWS), jnp.concatenate((x[whole:length, :].astype(F32), pad)), carry)
        out[whole:length, :] = total[: length - whole, :].astype(BF16)
    for i, value in enumerate(carry):
        sums[i : i + 1, :] = jnp.sum(value, axis=0, keepdims=True)


def lanes(shape):
    return lax.broadcasted_iota(jnp.int32, shape, 1)


def pick(ref, at):
    base = min(at // LANE * LANE, ref.shape[1] - 2 * LANE)
    window = ref[:, base : base + 2 * LANE]
    shift = at - base
    if shift:
        window = pltpu.roll(window, 2 * LANE - shift, 1)
    return window[:, :LANE]


def put(ref, at, value):
    base = min(at // LANE * LANE, ref.shape[1] - 2 * LANE)
    wide = jnp.concatenate((value, jnp.zeros_like(value)), axis=1)
    if at - base:
        wide = pltpu.roll(wide, at - base, 1)
    ref[:, base : base + 2 * LANE] += wide


def split3(value):
    hi = value.astype(BF16).astype(F32)
    rest = value - hi
    mid = rest.astype(BF16).astype(F32)
    return hi, mid, rest - mid


SCALE = HEAD ** -0.5
C2 = SCALE * math.log2(math.e)
PENALTY = -1e30


def attn_kernel(shapes, heads, length, chunk, group, final, *refs):
    n = shapes.num_leaves
    in1, mid_in, gain, shift = refs[:4]
    bias = refs[4:6]
    ab = nested(refs[6 : 6 + n], shapes)
    rest = refs[6 + n :]
    q_o, k_o, v_o, att_o = rest[0:2], rest[2:4], rest[4:6], rest[6:8]
    mid_o = rest[8]
    outs = 11 if final else 9
    in2_o, in2t_o = rest[9:11] if final else (None, None)
    in1_v, a_v, qkv_v, q_v, k_v, v_v, o_v, att_v, mid_v, attb_v, in2t_v, sems = rest[outs:]
    t, d = mid_v.shape
    c = Copies(sems)
    load_in = c(in1, in1_v)
    loads = [load_rows(c, ab[u], a_v.at[u]) for u in range(2)]
    load_mid = c(mid_in, mid_v)
    load_in.wait()
    part = HEAD * heads
    stores = [[pltpu.make_async_copy(src.at[u], dst[u], sems.at[c.n + 4 * u + i])
               for i, (src, dst) in enumerate(((k_v, k_o), (v_v, v_o), (q_v, q_o), (attb_v, att_o)))] for u in range(2)]

    def slot(u, _):
        for k in range(2):
            @pl.when(u == k)
            def _():
                wait(loads[k])

        bias_row = jnp.where(u == 0, bias[0][0:1, :], bias[1][0:1, :])
        for a in range(0, 7 * LANE, 512):
            w = min(512, 7 * LANE - a)
            qkv_v[:, a : a + w] = (dot(in1_v[...], a_v[u, :, a : a + w]) + bias_row[:, a : a + w]).astype(BF16)
        lane = lanes((t, LANE))
        row = lax.broadcasted_iota(jnp.int32, (t, LANE), 0)
        tail_k = jnp.where(lane < HEAD + 3, 1.0, jnp.where((lane == HEAD + 3) & (row >= length), 1.0, 0.0))
        tail_q = jnp.where(lane == HEAD + 3, PENALTY, 0.0)
        tail_v = jnp.where(lane < HEAD + 2, 1.0, 0.0)
        for j in range(heads):
            q_v[u, j] = jnp.where(lane < HEAD, pick(qkv_v, HEAD * j).astype(F32), tail_q).astype(BF16)
            k_v[u, j] = jnp.where(lane < HEAD, pick(qkv_v, part + HEAD * j).astype(F32), tail_k).astype(BF16)
            v_v[u, j] = jnp.where(lane < HEAD, pick(qkv_v, 2 * part + HEAD * j).astype(F32), tail_v).astype(BF16)
        for k in range(2):
            @pl.when(u == k)
            def _():
                stores[k][0].start()
                stores[k][1].start()

        ln = lanes((chunk, LANE))

        def head(g, _):
            def rows(i, _):
                at = pl.ds(pl.multiple_of(i * chunk, 16), chunk)
                for r in range(group):
                    j = g * group + r
                    q = q_v[u, j, at, :]
                    s = dot_nt(q, k_v[u, j])
                    m = jnp.max(s, axis=1, keepdims=True)
                    p = jnp.exp2((s - m) * C2)
                    o = dot(p.astype(BF16), v_v[u, j])
                    total = jnp.sum(jnp.where(ln == HEAD, o, 0.0), axis=1, keepdims=True)
                    o_v[j, at, :] = jnp.where(ln < HEAD, o / total, 0.0).astype(BF16)
                    hi, mid, lo = split3(m + jnp.log2(total) * (1.0 / C2))
                    aug = jnp.where(ln == HEAD, -hi, jnp.where(ln == HEAD + 1, -mid, jnp.where(ln == HEAD + 2, -lo, q.astype(F32))))
                    q_v[u, j, at, :] = aug.astype(BF16)
                return 0

            return lax.fori_loop(0, t // chunk, rows, 0)

        lax.fori_loop(0, heads // group, head, 0)
        att_v[...] = jnp.zeros_like(att_v)
        for j in range(heads):
            put(att_v, 3 * LANE - part + HEAD * j, o_v[j])
        attb_v[u] = att_v[...]
        for k in range(2):
            @pl.when(u == k)
            def _():
                stores[k][2].start()
                stores[k][3].start()

        @pl.when(u == 0)
        def _():
            load_mid.wait()

        for a in range(0, d, 512):
            w = min(512, d - a)
            mid_v[:, a : a + w] += dot_nt(attb_v[u], a_v[u, a : a + w, 6 * LANE : 9 * LANE])
        return 0

    lax.fori_loop(0, 2, slot, 0)
    last = Copies(sems)
    last.n = c.n + 8
    done = [last(mid_v, mid_o)]
    if final:
        def norm(at, _):
            value = mid_v[at, :]
            average, inverse = stats(value)
            in1_v[at, :] = ((value - average) * inverse * gain[...] + shift[...]).astype(BF16)
            return 0

        row_loop(t, norm, 0)
        done.append(last(in1_v, in2_o))
        turn(in2t_v, in1_v)
        done.append(last(in2t_v, in2t_o))
    wait(done)
    for k in range(2):
        wait(stores[k])


def attn(in1, biases, ab, mid, gain, shift, length, final, chunk=368, group=1):
    blocks, shapes = jax.tree.flatten(ab)
    n, (t, d) = len(blocks), in1.shape
    w = blocks[0].shape[1]
    heads = w // 4 // HEAD
    tp = -(-t // LANE) * LANE
    o = jax.ShapeDtypeStruct
    hs = (heads, t, LANE)
    return pl.pallas_call(
        functools.partial(attn_kernel, shapes, heads, length, chunk, group, final),
        name="attn",
        in_specs=[ANY, ANY, VM, VM, VM, VM] + [ANY] * n,
        out_specs=[ANY] * (11 if final else 9),
        out_shape=[o(hs, BF16)] * 6 + [o((t, 3 * LANE), BF16)] * 2 + [o((t, d), F32)] + ([o((t, d), BF16), o((d, tp), BF16)] if final else []),
        scratch_shapes=[
            pltpu.VMEM((t, d), BF16), pltpu.VMEM((2, d, w), BF16), pltpu.VMEM((t, 8 * LANE), BF16),
            pltpu.VMEM((2, *hs), BF16), pltpu.VMEM((2, *hs), BF16), pltpu.VMEM((2, *hs), BF16), pltpu.VMEM(hs, BF16),
            pltpu.VMEM((t, 3 * LANE), BF16), pltpu.VMEM((t, d), F32), pltpu.VMEM((2, t, 3 * LANE), BF16),
            pltpu.VMEM((d, tp) if final else (16, LANE), BF16),
            pltpu.SemaphoreType.DMA((n + 14,)),
        ],
        input_output_aliases={1: 8},
        compiler_params=pltpu.CompilerParams(vmem_limit_bytes=VLIM),
        cost_estimate=pl.CostEstimate(flops=4 * t * d * w + 16 * heads * t * t * LANE, bytes_accessed=4 * d * w + 20 * t * d, transcendentals=2 * heads * t * t),
    )(in1, mid, gain, shift, *biases, *blocks)


GC = math.sqrt(2.0 / math.pi)


def ff_kernel(shapes, length, final, *refs):
    n = shapes.num_leaves
    in2, cot, mid, last, gain, sbias = refs[:6]
    bias = refs[6:8]
    eb, sb = nested(refs[8 : 8 + n], shapes)
    rest = refs[8 + n :]
    hid_o, gb_o, db = rest[0:2], rest[2:4], rest[4]
    if final:
        res_in, gi_in = mid, last
        result, gm32_o, gm_o, gmt_o, sums = rest[5:10]
        rest = rest[10:]
    else:
        res_o, gi_o = rest[5:7]
        rest = rest[7:]
    in2_v, cot_v, e_v, s_v, hid_v, gb_v, res_v, gi_v, mid_v, gmt_v, sems = rest
    t, d = in2_v.shape
    width = e_v.shape[2]
    c = Copies(sems)
    load_in = c(in2, in2_v)
    loads_e = [load_rows(c, eb[0], e_v.at[0])]
    load_cot = c(cot, cot_v)
    loads_s = [load_rows(c, sb[0], s_v.at[0])]
    loads_e.append(load_rows(c, eb[1], e_v.at[1]))
    loads_s.append(load_rows(c, sb[1], s_v.at[1]))
    if final:
        load_acc = [c(res_in[0], res_v), c(gi_in, gi_v)]
        load_mid = c(res_in[1], mid_v)
    else:
        load_acc = [c(mid, res_v)]
        gi_v[...] = jnp.zeros_like(gi_v)
    stores = [[pltpu.make_async_copy(src.at[u], dst[u], sems.at[c.n + 2 * u + i])
               for i, (src, dst) in enumerate(((hid_v, hid_o), (gb_v, gb_o)))] for u in range(2)]
    load_in.wait()

    def slot(u, _):
        for k in range(2):
            @pl.when(u == k)
            def _():
                wait(loads_e[k])
                if k == 0:
                    load_cot.wait()
                wait(loads_s[k])

        bias_row = jnp.where(u == 0, bias[0][1:2, :], bias[1][1:2, :])
        for a in range(0, width, 256):
            w = min(256, width - a)
            b = dot(in2_v[...], e_v[u, :, a : a + w]) + bias_row[:, a : a + w]
            sq = b * b
            th = jnp.tanh(GC * b * (1.0 + 0.044715 * sq))
            half = 0.5 * (1.0 + th)
            hid_v[u, :, a : a + w] = (b * half).astype(BF16)
            slope = half + (0.5 * GC) * b * (1.0 - th * th) * (1.0 + (3 * 0.044715) * sq)
            g = dot(cot_v[...], s_v[u, :, a : a + w]) * slope
            gb_v[u, :, a : a + w] = g.astype(BF16)
            db[u, :, a : a + w] = jnp.sum(g, axis=0, keepdims=True)
        for k in range(2):
            @pl.when(u == k)
            def _():
                for copy in stores[k]:
                    copy.start()
                if k == 0:
                    wait(load_acc)

        for a, w in ((0, d // 256 * 128), (d // 256 * 128, d - d // 256 * 128)):
            res_v[:, a : a + w] += dot_nt(hid_v[u], s_v[u, a : a + w, :])
            gi_v[:, a : a + w] += dot_nt(gb_v[u], e_v[u, a : a + w, :])
        return 0

    lax.fori_loop(0, 2, slot, 0)
    more = Copies(sems)
    more.n = c.n + 4
    if not final:
        done = [more(res_v, res_o), more(gi_v, gi_o)]
    else:
        load_mid.wait()
        whole = length // ROWS * ROWS
        zero = jnp.zeros((8, d), F32)

        def rows(at, carry):
            g, ct = gi_v[at, :], cot_v[at, :].astype(F32)
            inner, product = back_row(mid_v[at, :], g, gain[...])
            total = ct + inner
            mid_v[at, :] = total
            in2_v[at, :] = total.astype(BF16)
            return tuple(x + fold(y) for x, y in zip(carry, (total, product, g, ct)))

        def step(at, carry):
            result[at, :] = (res_v[at, :] + sbias[...]).astype(BF16)
            return rows(at, carry)

        carry = row_loop(whole, step, (zero,) * 4)
        if whole < t:
            value = (res_v[whole:t, :] + sbias[...]).astype(BF16)
            result[whole:length, :] = value[: length - whole, :]
            carry = rows(pl.ds(whole, ROWS), carry)
        for i, value in enumerate(carry):
            sums[i : i + 1, :] = jnp.sum(value, axis=0, keepdims=True)
        done = [more(mid_v, gm32_o), more(in2_v, gm_o)]
        turn(gmt_v, in2_v)
        done.append(more(gmt_v, gmt_o))
    wait(done)
    for k in range(2):
        wait(stores[k])


def ff(in2, cot, mid, acc, gain, sbias, biases, eb, sb, length):
    final = acc is not None
    blocks, shapes = jax.tree.flatten((eb, sb))
    n, (t, d) = len(blocks), in2.shape
    w = blocks[0].shape[1]
    tp = -(-t // LANE) * LANE
    o = jax.ShapeDtypeStruct
    outs = [o((t, w), BF16)] * 4 + [o((2, 1, w), F32)]
    specs = [ANY] * 4 + [VM]
    if final:
        outs += [o((length, d), BF16), o((t, d), F32), o((t, d), BF16), o((d, tp), BF16), o((4, d), F32)]
        specs += [VM, ANY, ANY, ANY, VM]
        args = (in2, cot, acc[0], mid, acc[1], gain, sbias)
    else:
        outs += [o((t, d), F32)] * 2
        specs += [ANY] * 2
        args = (in2, cot, mid, gain, sbias)

    def body(*refs):
        if final:
            ff_kernel(shapes, length, True, refs[0], refs[1], (refs[2], refs[3]), refs[4], *refs[5:])
        else:
            ff_kernel(shapes, length, False, refs[0], refs[1], refs[2], None, *refs[3:])

    return pl.pallas_call(
        body,
        name="ff",
        in_specs=[ANY] * (len(args) - 2) + [VM] * 4 + [ANY] * n,
        out_specs=specs,
        out_shape=outs,
        scratch_shapes=[
            pltpu.VMEM((t, d), BF16), pltpu.VMEM((t, d), BF16),
            pltpu.VMEM((2, d, w), BF16), pltpu.VMEM((2, d, w), BF16),
            pltpu.VMEM((2, t, w), BF16), pltpu.VMEM((2, t, w), BF16),
            pltpu.VMEM((t, d), F32), pltpu.VMEM((t, d), F32),
            pltpu.VMEM((t, d) if final else (8, LANE), F32), pltpu.VMEM((d, tp) if final else (16, LANE), BF16),
            pltpu.SemaphoreType.DMA((n + 14,)),
        ],
        compiler_params=pltpu.CompilerParams(vmem_limit_bytes=VLIM),
        cost_estimate=pl.CostEstimate(flops=16 * t * d * w, bytes_accessed=8 * d * w + 24 * t * d, transcendentals=2 * t * w),
    )(*args, *biases, *blocks)


def back_kernel(shape, heads, chunk, group, first, final, *refs):
    n = shape.num_leaves
    gm = refs[0]
    ab = nested(refs[1 : 1 + n], shape)
    q_i, k_i, v_i, att_i = refs[1 + n : 5 + n]
    rest = refs[5 + n :]
    if not first:
        gi_in, rest = rest[0], rest[1:]
    if final:
        x, gm32, gain = rest[:3]
        rest = rest[3:]
    dqkv_o, db = rest[:2]
    if final:
        out, sums = rest[2:4]
    else:
        gi_o = rest[2]
    rest = rest[4:] if final else rest[3:]
    gm_v, a_v, ga_v, q_v, k_v, v_v, g_v, att_v, ds_v, dq_v, dk_v, dv_v, pack_v, gi_v, gm32_v, sems = rest
    t, d = gi_v.shape
    c = Copies(sems)
    begin = [c(gm, gm_v)] + load_rows(c, ab, a_v)
    second = [c(att_i, att_v), c(q_i, q_v), c(k_i, k_v), c(v_i, v_v)]
    if first:
        third = []
        gi_v[...] = jnp.zeros_like(gi_v)
    else:
        third = [c(gi_in, gi_v)]
    if final:
        third.append(c(gm32, gm32_v))
    pack_v[...] = jnp.zeros_like(pack_v)
    wait(begin)
    ga_v[...] = dot(gm_v[...], a_v[:, 6 * LANE : 9 * LANE]).astype(BF16)
    lane = lanes((t, LANE))
    wide = lanes((t, 2 * LANE))
    part = HEAD * heads
    wait(second)
    for j in range(heads):
        at = 3 * LANE - part + HEAD * j
        base = min(at // LANE * LANE, LANE)
        window = ga_v[:, base : base + 2 * LANE].astype(F32) * att_v[:, base : base + 2 * LANE].astype(F32)
        inside = (wide >= at - base) & (wide < at - base + HEAD)
        delta = jnp.sum(jnp.where(inside, window, 0.0), axis=1, keepdims=True)
        hi = delta.astype(BF16).astype(F32)
        g = pick(ga_v, at).astype(F32)
        g_v[j] = jnp.where(lane < HEAD, g, jnp.where(lane == HEAD, -hi, jnp.where(lane == HEAD + 1, hi - delta, 0.0))).astype(BF16)

    def head(h, _):
        def rows(i, _):
            at = pl.ds(pl.multiple_of(i * chunk, 16), chunk)
            for r in range(group):
                j = h * group + r
                p = jnp.exp2(dot_nt(k_v[j, at, :], q_v[j]) * C2)
                ds = (p * dot_nt(v_v[j, at, :], g_v[j])).astype(BF16)
                dv_v[j, at, :] = dot(p.astype(BF16), g_v[j]).astype(BF16)
                dk_v[j, at, :] = (dot(ds, q_v[j]) * SCALE).astype(BF16)
                ds_v[r, at, :] = ds
            return 0

        lax.fori_loop(0, t // chunk, rows, 0)
        for r in range(group):
            j = h * group + r
            dq_v[j] = (dot_tn(ds_v[r], k_v[j]) * SCALE).astype(BF16)
        return 0

    lax.fori_loop(0, heads // group, head, 0)
    for j in range(heads):
        for i, ref in enumerate((dq_v, dk_v, dv_v)):
            put(pack_v, i * part + HEAD * j, jnp.where(lane < HEAD, ref[j].astype(F32), 0.0).astype(BF16))
    more = Copies(sems)
    more.n = c.n
    done = [more(pack_v, dqkv_o)]
    db[...] = jnp.sum(pack_v[...].astype(F32), axis=0, keepdims=True)
    wait(third)
    for a in range(0, d, 512):
        w = min(512, d - a)
        gi_v[:, a : a + w] += dot_nt(pack_v[...], a_v[a : a + w, : 7 * LANE])
    if final:
        leave_body(gi_v, x, gm32_v, gain, out, sums)
    else:
        done.append(more(gi_v, gi_o))
    wait(done)


def back(gm, ab, q, k, v, att, gi, leaving=None, chunk=368, group=4):
    blocks, shape = jax.tree.flatten(ab)
    n, (t, d) = len(blocks), gm.shape
    w = blocks[0].shape[1]
    heads = q.shape[0]
    first, final = gi is None, leaving is not None
    o = jax.ShapeDtypeStruct
    hs = (heads, t, LANE)
    args, specs = (gm, *blocks, q, k, v, att), [ANY] * (n + 5)
    if not first:
        args, specs = (*args, gi), specs + [ANY]
    outs, out_specs = [o((t, 7 * LANE), BF16), o((1, 7 * LANE), F32)], [ANY, VM]
    if final:
        args, specs = (*args, *leaving), specs + [VM, ANY, VM]
        outs, out_specs = outs + [o(leaving[0].shape, BF16), o((2, d), F32)], out_specs + [VM, VM]
    else:
        outs, out_specs = outs + [o((t, d), F32)], out_specs + [ANY]
    return pl.pallas_call(
        functools.partial(back_kernel, shape, heads, chunk, group, first, final),
        name="back",
        in_specs=specs,
        out_specs=out_specs,
        out_shape=outs,
        scratch_shapes=[
            pltpu.VMEM((t, d), BF16), pltpu.VMEM((d, w), BF16), pltpu.VMEM((t, 3 * LANE), BF16),
            pltpu.VMEM(hs, BF16), pltpu.VMEM(hs, BF16), pltpu.VMEM(hs, BF16), pltpu.VMEM(hs, BF16),
            pltpu.VMEM((t, 3 * LANE), BF16), pltpu.VMEM((group, t, t), BF16),
            pltpu.VMEM(hs, BF16), pltpu.VMEM(hs, BF16), pltpu.VMEM(hs, BF16),
            pltpu.VMEM((t, 7 * LANE), BF16), pltpu.VMEM((t, d), F32), pltpu.VMEM((t, d) if final else (8, LANE), F32),
            pltpu.SemaphoreType.DMA((n + 10,)),
        ],
        compiler_params=pltpu.CompilerParams(vmem_limit_bytes=VLIM),
        cost_estimate=pl.CostEstimate(flops=2 * t * d * w + 20 * heads * t * t * LANE, bytes_accessed=2 * d * w + 16 * t * d, transcendentals=heads * t * t),
    )(*args)


def grads_kernel(n, split, groups, *refs):
    k = len(groups)
    ins = refs[: 4 * k]
    outs = refs[4 * k : 4 * k + n]
    scratch = refs[4 * k + n :]
    lhs, rhs = scratch[: 2 * k], scratch[2 * k : 4 * k]
    acc, tile_v, sems, osem = scratch[4 * k :]
    c = Copies(sems)
    cps = []
    for i in range(k):
        cps += [c(ins[4 * i + u], (lhs if u < 2 else rhs)[2 * i + u % 2]) for u in range(4)]
    wait(cps)
    size = outs[0].shape[0]
    t = rhs[0].shape[0]
    me = lax.axis_index("row")

    def step(s, _):
        slot = lax.rem(s, 2)
        row = pl.multiple_of(lax.rem(me * split + s, n) * size, 16)
        rows = pl.ds(row, size)

        @pl.when(s >= 2)
        def _():
            pltpu.make_async_copy(tile_v.at[slot], outs[0], osem.at[slot]).wait()

        if k == 1:
            def body(at):
                cols = pl.ds(at, 256)
                tile_v[slot, :, cols] = (
                    dot(lhs[0][rows, :t], rhs[0][:, cols]) + dot(lhs[1][rows, :t], rhs[1][:, cols])
                ).astype(BF16)

            tiles(groups[0][1], 256, body)
        else:
            for i, (start, width) in enumerate(groups):
                done = 0 if i == 0 else groups[i - 1][0] + groups[i - 1][1]
                for a in range(0, width, 256):
                    w = min(256, width - a)
                    value = dot(lhs[2 * i][rows, :t], rhs[2 * i][:, a : a + w]) + dot(
                        lhs[2 * i + 1][rows, :t], rhs[2 * i + 1][:, a : a + w]
                    )
                    at = start + a
                    if at < done:
                        o = done - at
                        value = jnp.concatenate((value[:, :o] + acc[:, at : at + o], value[:, o:]), axis=1) if o < w else value + acc[:, at : at + w]
                    acc[:, at : at + w] = value
            tile_v[slot] = acc[...].astype(BF16)
        for u in range(n):
            @pl.when(s == u)
            def _():
                pltpu.make_async_copy(tile_v.at[slot], outs[u], osem.at[slot]).start()
        return 0

    lax.fori_loop(0, n, step, 0)
    for u in range(max(0, n - 2), n):
        pltpu.make_async_copy(tile_v.at[u % 2], outs[u], osem.at[u % 2]).wait()


def grads(n, terms, width, split=1):
    k = len(terms)
    groups = tuple((term[0], term[3].shape[1]) for term in terms)
    flat = [array for term in terms for array in term[1:]]
    d, t = terms[0][1].shape[0], terms[0][3].shape[0]
    n = n * split
    size = d // n
    scratch = [pltpu.VMEM(term[1].shape, BF16) for term in terms for _ in range(2)]
    scratch += [pltpu.VMEM(term[3].shape, BF16) for term in terms for _ in range(2)]
    flops = sum(4 * d * t * w for _, w in groups)
    return pl.pallas_call(
        functools.partial(grads_kernel, n, split, groups),
        name="grads",
        in_specs=[ANY] * (4 * k),
        out_specs=[ANY] * n,
        out_shape=[jax.ShapeDtypeStruct((size, width), BF16)] * n,
        scratch_shapes=scratch + [
            pltpu.VMEM((size, width if k > 1 else LANE), F32), pltpu.VMEM((2, size, width), BF16),
            pltpu.SemaphoreType.DMA((4 * k,)), pltpu.SemaphoreType.DMA((2,)),
        ],
        compiler_params=pltpu.CompilerParams(vmem_limit_bytes=VLIM),
        cost_estimate=pl.CostEstimate(flops=flops, bytes_accessed=2 * d * width + 8 * t * d, transcendentals=0),
    )(*flat)


CORE, SIDE = 1, 2


def hop_row(value, shift, size):
    return lax.ppermute(value, "row", [(i, (i + shift) % size) for i in range(size)])


def hop_col(value, flip):
    return lax.ppermute(value, "col", [(i, i ^ flip) for i in range(4)])


def hop_dp(value, flip):
    return lax.ppermute(value, "dp", [(i, i ^ flip) for i in range(4)])


def after(value, *first):
    return lax.optimization_barrier((value, *first))[0]


def near(block, n):
    return [block] + [hop_row(block, s, n) for s in range(1, n)], hop_col(block, SIDE)


def diagonal(own, side, n, via):
    parts = [side]
    half = side.shape[0] // 2
    for s in range(1, n):
        if via == "row":
            parts.append(hop_row(side, s, n))
        elif via == "col":
            parts.append(hop_col(own[s], SIDE))
        else:
            parts.append((hop_row(side[:half], s, n), hop_col(own[s][half:], SIDE)))
    return parts


def across(parts):
    return [jax.tree.map(lambda b: hop_col(b, CORE), part) for part in parts]


def add(a, b):
    return (a.astype(F32) + b.astype(F32)).astype(BF16)


def over_row(parts, n):
    total = parts[0]
    for s in range(1, n):
        total = add(total, hop_row(parts[s], s, n))
    return total


def over_dp(total):
    half = total.shape[0] // 2
    low = lax.rem(lax.axis_index("dp"), 2)
    mine = lax.dynamic_slice_in_dim(total, low * half, half, 0)
    theirs = lax.dynamic_slice_in_dim(total, (1 - low) * half, half, 0)
    mine = add(mine, hop_dp(theirs, 1))
    mine = add(mine, hop_dp(mine, 2))
    return mine, hop_dp(mine, 1)


def joined_halves(mine, theirs):
    even = lax.rem(lax.axis_index("dp"), 2) == 0
    return jnp.where(even, jnp.concatenate((mine, theirs)), jnp.concatenate((theirs, mine))).astype(F32)


def layer(n, images, cotangent, first_gain, first_shift, query_weight, query_bias, key_weight, value_weight, value_bias,
          output_weight, output_bias, second_gain, second_shift, expand_weight, expand_bias, shrink_weight, shrink_bias):
    length, d = images.shape[1:]
    t = -(-length // 16) * 16
    part, ff_part = query_weight.shape[1], expand_weight.shape[1]
    wide = 4 * part
    pad_ff = ((0, 0), (0, wide - ff_part))
    a_own = weave(query_weight.T, key_weight.T, value_weight.T, output_weight)
    zeros = jnp.zeros((part,), F32)
    bias_own = jnp.stack((jnp.concatenate((query_bias, zeros, value_bias, zeros)), jnp.pad(expand_bias, pad_ff[1:])))
    a_near, a_side = near(a_own, n)
    bias_side = hop_col(bias_own, SIDE)
    biases = [bias_own, bias_side, hop_col(bias_own, CORE), hop_col(bias_side, CORE)]
    row = lambda v: v.reshape(1, -1)
    images, cotangent = images[0], cotangent[0]
    input1, in1_t, cot, cot_t, middle = enter(
        after(images, a_own), cotangent, row(first_gain), row(first_shift), row(output_bias), t)
    e_own = jnp.pad(expand_weight, pad_ff)
    s_own = jnp.pad(shrink_weight.T, pad_ff)

    a_far = diagonal(a_near, a_side, n, "both")
    a_all = [a_near, a_far, across(a_near), across(a_far)]
    e_near, e_side = near(after(e_own, a_side), n)
    s_near, s_side = near(after(s_own, a_side), n)
    e_far = diagonal(e_near, e_side, n, "row")
    s_far = diagonal(s_near, s_side, n, "col")
    e_all = [e_near, e_far, across(e_near), across(e_far)]
    s_all = [s_near, s_far, across(s_near), across(s_far)]
    cot_t2 = hop_col(after(cot_t, a_side), CORE)
    in1_t2 = hop_col(after(in1_t, a_side), CORE)

    gain2, shift2 = row(second_gain), row(second_shift)
    kept = {}

    def attend(pair, last, middle, final):
        out = attn(input1, [after(biases[pair], last), biases[pair + 2]], [a_all[pair], a_all[pair + 2]],
                  middle, gain2, shift2, length, final)
        for i in range(2):
            kept[pair + 2 * i] = (out[i], out[2 + i], out[4 + i], out[6 + i])
        return out[8:]

    middle, = attend(0, middle, middle, False)
    middle, input2, in2_t = attend(1, kept[0][3], middle, True)
    in2_t2 = hop_col(in2_t, CORE)
    att2 = [hop_col(kept[s + 2][3], CORE) for s in (0, 1)]
    hidden, before, expand_sums, ge, gs = {}, {}, {}, {}, {}

    def feed(pair, last, acc):
        out = ff(input2, cot, middle, acc, gain2, row(shrink_bias), [after(biases[pair], last), biases[pair + 2]],
                  [e_all[pair], e_all[pair + 2]], [s_all[pair], s_all[pair + 2]], length)
        for i in range(2):
            hidden[pair + 2 * i], before[pair + 2 * i], expand_sums[pair + 2 * i] = out[i], out[2 + i], out[4][i]
        return out[5:]

    def expand_grads(slot, last):
        other = hop_col(before[slot + 2], CORE)
        ge[slot] = grads(n, [(0, in2_t, in2_t2, after(before[slot], last), other)], wide)
        return ge[slot][-1]

    def shrink_grads(slot, last):
        other = hop_col(hidden[slot + 2], CORE)
        gs[slot] = grads(n, [(0, cot_t, cot_t2, after(hidden[slot], last), other)], wide)
        return gs[slot][-1]

    acc = feed(0, in2_t, None)
    last = expand_grads(0, expand_sums[0])
    result, gm32, gm, gm_t, middle_sums = feed(1, last, acc)
    gm_t2 = hop_col(gm_t, CORE)
    last = expand_grads(1, middle_sums)
    last = shrink_grads(0, last)
    last = shrink_grads(1, last)
    joined, joined_sums, ga = {}, {}, {}

    def attend_back(slot, last, grad1, leaving=None):
        q, k, v, att = kept[slot]
        joined[slot], joined_sums[slot], *out = back(
            gm, a_all[slot], q, k, v, after(att, last), grad1, leaving)
        return out

    def joined_grads(slot, last, split=1):
        other = hop_col(joined[slot + 2], CORE)
        ga[slot] = grads(n, [
            (0, in1_t, in1_t2, after(joined[slot], last), other),
            (wide - 384, gm_t, gm_t2, kept[slot][3], att2[slot]),
        ], wide, split)
        return ga[slot][-1]

    grad1, = attend_back(3, last, None)
    grad1, = attend_back(1, joined_sums[3], grad1)
    grad1, = attend_back(2, joined_sums[1], grad1)
    last = joined_grads(1, joined_sums[2])
    grad_stream, first_sums = attend_back(0, last, grad1, (images, gm32, row(first_gain)))
    split = 2 if d // n % 32 == 0 else 1
    joined_grads(0, first_sums, split)

    e_total = over_dp(add(over_row(ge[0], n), hop_col(over_row(ge[1], n), SIDE)))
    s_total = over_dp(add(over_row(gs[0], n), hop_col(over_row(gs[1], n), SIDE)))
    a_side = hop_col(over_row(ga[1], n), SIDE)
    piece = a_side.shape[0] // split
    a_total = []
    for i in range(split):
        total = add(ga[0][i], a_side[i * piece : (i + 1) * piece])
        for s in range(1, n):
            total = add(total, hop_row(ga[0][s * split + i], s, n))
        a_total.append(over_dp(total))
    fill = lambda rows, count: jnp.pad(rows, ((0, count - rows.shape[0]), (0, 0)))
    sums = [jnp.concatenate((jnp.pad(joined_sums[s], ((0, 0), (0, wide - joined_sums[s].shape[1]))), expand_sums[s])) for s in range(4)]
    features = fill(jnp.concatenate((first_sums, middle_sums)), 6)
    two = jnp.concatenate((features, sums[0], sums[1])) + hop_col(jnp.concatenate((features, sums[2], sums[3])), CORE)
    one = two[:8] + hop_col(jnp.concatenate((two[:6], two[8:])), SIDE)
    total = one
    for s in range(1, n):
        total = total + hop_row(one, s, n)
    for flip in (1, 2):
        total = total + hop_dp(total, flip)
    biases = total[6:]
    gq, gk, gv, go = unweave(a_total, part)
    return (
        result[None],
        grad_stream[None],
        total[0],
        total[1],
        gq.T,
        biases[0, :part],
        gk.T,
        gv.T,
        biases[0, 2 * part : 3 * part],
        go,
        total[2],
        total[3],
        total[4],
        joined_halves(*e_total)[:, :ff_part],
        biases[1, :ff_part],
        joined_halves(*s_total)[:, :ff_part].T,
        total[5],
    )


def solution(mesh):
    batch = P(("dp", "row", "col"), None, None)
    into, out, cols, whole = P("row", "col"), P("col", "row"), P("col"), P()

    def step(*args):
        return layer(mesh.shape["row"], *args)

    return jax.shard_map(
        step,
        mesh=mesh,
        in_specs=(batch, batch, whole, whole, into, cols, into, into, cols, out, whole, whole, whole, into, cols, out, whole),
        out_specs=(batch, batch, whole, whole, into, cols, into, into, cols, out, whole, whole, whole, into, cols, out, whole),
        check_vma=False,
    )
```
